256 devices in a mesh: dp: 16 (over z_lo, x, core), tensor: 16 (over z_hi, y).
Axes of the slice: x: 4, y: 4, z: 8 (z_hi: 4, z_lo: 2; z = z_hi * 2 + z_lo), core: 2. Of those that a mesh axis runs over, the one named last changes fastest.
Arguments:
- activations: bfloat16 [4096, 5120], P('dp'), may hold values from -6 to 6
- grad_out: bfloat16 [4096, 5120], P('dp'), may hold values from -6 to 6
- gate_pre: bfloat16 [4096, 7168], P('dp', 'tensor'), may hold values from -8 to 8
- up_pre: bfloat16 [4096, 7168], P('dp', 'tensor'), may hold values from -6 to 6
- gate_up: bfloat16 [5120, 2, 7168], P('dp', None, 'tensor'), may hold values from -0.078125 to 0.078125
- down_weight: bfloat16 [5120, 7168], P('dp', 'tensor'), may hold values from -0.0625 to 0.0625
Outputs:
- grad_input: bfloat16 [4096, 5120], P('dp')
- grad_gate_up: float32 [5120, 2, 7168], P('dp', None, 'tensor')
- grad_down: float32 [5120, 7168], P('dp', 'tensor')
The draws below stay inside these ranges and needn't reach their ends.
All inputs are finite; a program needn't handle non-finite values.
Results may differ from the reference program's by a relative error of at most 0.017.
Values may be sent and summed in bfloat16 or wider, within the bound.
A program may use at most 128 MiB of HBM per device.

```python
import jax
import jax.numpy as jnp
from jax import lax

D = 5120
FF = 7168
TOK_DEV = 256
TOKENS = 4096
N_DP = 16
N_TENSOR = 16


def raised(result, stream_key, source, target, blocks, factor):
    owner, partner = [(jnp.arange(result.shape[dim]) // (result.shape[dim] // blocks)).reshape([-1 if axis == dim else 1 for axis in range(result.ndim)]) for dim in (source, target)]
    chosen = jax.random.permutation(stream_key, blocks)[partner]
    strong = (owner == chosen) | (owner == (partner + blocks // 2) % blocks)
    return jnp.where(strong, factor * result, result)


def shard_levels(own_key, extent, cuts, low, high):
    def one(dim, shards_of):
        draws = jax.random.uniform(jax.random.fold_in(jax.random.fold_in(own_key, 6), dim), (shards_of,), jnp.float32, low / len(cuts), high / len(cuts))
        return jnp.repeat(jnp.exp(draws), extent[dim] // shards_of).reshape((-1,) + (1,) * (len(extent) - dim - 1))

    gain = one(*cuts[0])
    for cut in cuts[1:]:
        gain = gain * one(*cut)
    return gain


def scatter_about(own_key, dims, scale, bound, shards=(), kind=jnp.bfloat16):
    array = jax.random.normal(own_key, dims, jnp.float32) * scale
    if len(shards) > 0:
        array = shard_levels(own_key, dims, shards, -0.22, 0.18) * array
    return jnp.clip(array, min=-bound, max=bound).astype(kind)


def gaussian_with(key, shape, scale, bound, split, heavy, kind=jnp.bfloat16):
    drawn = scale * jax.random.normal(key, shape, jnp.float32)
    if split:
        drawn = drawn * shard_levels(key, shape, split, -0.22, 0.18)
    return jnp.clip(raised(drawn, jax.random.fold_in(key, 3), *heavy), -bound, bound).astype(kind)


def setup_inputs(seed: int = 0) -> dict:
    key_list = jax.random.split(jax.random.key(seed), 7)
    return {
        "activations": gaussian_with(key_list[0], (TOKENS, D), 1.0, 6.0, ((0, 16),), (0, 1, 16, 2.0)),
        "grad_out": gaussian_with(key_list[1], (TOKENS, D), 1.0, 6.0, ((0, 16),), (0, 1, 16, 2.0)),
        "gate_pre": scatter_about(key_list[2], (TOKENS, FF), 1.5, 8.0, ((0, 16), (1, 16))),
        "up_pre": scatter_about(key_list[3], (TOKENS, FF), 1.0, 6.0, ((0, 16), (1, 16))),
        "gate_up": scatter_about(key_list[4], (D, 2, FF), D ** -0.5, 0.078125, ((0, 16), (2, 16))),
        "down_weight": scatter_about(key_list[5], (D, FF), FF ** -0.5, 0.0625, ((0, 16), (1, 16))),
    }


def reference(activations, grad_out, gate_pre, up_pre, gate_up, down_weight):
    gate_wide = gate_pre.astype(jnp.float32)
    up_wide = up_pre.astype(jnp.float32)
    gate_sigmoid = jax.nn.sigmoid(gate_wide)
    gate_silu = gate_wide * gate_sigmoid
    hidden = (gate_silu * up_wide).astype(jnp.bfloat16)
    grad_h = jnp.dot(grad_out, down_weight, preferred_element_type=jnp.float32)
    grad_gate = grad_h * up_wide * gate_sigmoid * (1.0 + gate_wide * (1.0 - gate_sigmoid))
    grad_up = grad_h * gate_silu
    grad_hidden = jnp.stack([grad_gate, grad_up], axis=1).astype(jnp.bfloat16)

    group_width = FF // N_TENSOR
    hidden_groups = grad_hidden.reshape(TOKENS, 2, N_TENSOR, group_width).transpose(2, 0, 1, 3)
    hidden_groups = hidden_groups.reshape(N_TENSOR, TOKENS, 2 * group_width)
    weight_groups = gate_up.reshape(D, 2, N_TENSOR, group_width).transpose(2, 0, 1, 3)
    weight_groups = weight_groups.reshape(N_TENSOR, D, 2 * group_width)

    def add_part(running, paired):
        left_rows, right_rows = paired
        part_sum = jnp.dot(left_rows, right_rows.T, preferred_element_type=jnp.float32)
        part_sum = lax.optimization_barrier(part_sum.astype(jnp.bfloat16))
        return running + part_sum.astype(jnp.float32), None

    input_total, _ = lax.scan(add_part, jnp.zeros((TOKENS, D), jnp.float32), (hidden_groups, weight_groups))
    grad_input = input_total.astype(jnp.bfloat16)

    act_groups = activations.reshape(N_DP, TOK_DEV, D)
    out_groups = grad_out.reshape(N_DP, TOK_DEV, D)
    grad_groups = grad_hidden.reshape(N_DP, TOK_DEV, 2 * FF)
    plain_groups = hidden.reshape(N_DP, TOK_DEV, FF)

    def add_group(running, group_items):
        act_rows, out_rows, grad_rows, plain_rows = group_items
        gate_part = jnp.dot(act_rows.T, grad_rows, preferred_element_type=jnp.float32)
        down_part = jnp.dot(out_rows.T, plain_rows, preferred_element_type=jnp.float32)
        gate_part = lax.optimization_barrier(gate_part.astype(jnp.bfloat16))
        down_part = lax.optimization_barrier(down_part.astype(jnp.bfloat16))
        return (running[0] + gate_part.astype(jnp.float32), running[1] + down_part.astype(jnp.float32)), None

    start_sums = (jnp.zeros((D, 2 * FF), jnp.float32), jnp.zeros((D, FF), jnp.float32))
    summed, _ = lax.scan(add_group, start_sums, (act_groups, out_groups, grad_groups, plain_groups))
    grad_gate_up = (summed[0] / N_DP).reshape(D, 2, FF)
    grad_down = summed[1] / N_DP
    return grad_input, grad_gate_up, grad_down
```

```python
import jax
import jax.numpy as jnp
from jax import lax
from jax.experimental import pallas as pl
from jax.experimental.pallas import tpu as pltpu
from jax.sharding import Mesh
from jax.sharding import PartitionSpec as P

Z, X, C, H, Y = "dp_0", "dp_1", "dp_2", "tensor_0", "tensor_1"
DP = (Z, X, C)
TENSOR = (H, Y)
BF = jnp.bfloat16
F32 = jnp.float32

TOK = 256
D = 5120
DH = D // 2
SLAB = 640
ROWS = 320
HALF = 160
FD = 448
FG = 896
QT = 64
HT = 16


class Sems:
    def __init__(self):
        self.n = 0

    def block(self, count=1):
        first = self.n
        self.n += count
        return first


def wgrad_slab(acts, right, xs):
    cols = pl.ds(pl.multiple_of(xs * SLAB, 128), SLAB)
    return lax.dot_general(
        acts[:, cols], right[...], (((0,), (0,)), ((), ())), preferred_element_type=F32
    )


def kernel(
    a_hbm,
    g_hbm,
    gp_hbm,
    up_hbm,
    gu_hbm,
    dn_hbm,
    gi_hbm,
    wg_out,
    wd_out,
    gb,
    ab,
    wd,
    wg,
    gpt,
    upt,
    ghf,
    ghs,
    ghr,
    silu_s,
    dgate_s,
    hid,
    ghb,
    dws_d,
    dwr_d,
    dws_g,
    dwr_g,
    vs_d,
    vs_g,
    r1_d,
    r1_g,
    r2_d,
    r2_g,
    pb,
    r1p,
    r1m,
    r2p,
    r2m,
    yb,
    zr,
    ob,
    lsem,
    ss,
    rs,
):
    l, x, c, h, y = (lax.axis_index(n) for n in (Z, X, C, H, Y))
    xp, xm, xo = (x + 1) % 4, (x + 3) % 4, (x + 2) % 4
    yp, ym, yo = (y + 1) % 4, (y + 3) % 4, (y + 2) % 4
    to_xp, to_xm = {X: xp}, {X: xm}
    to_yp, to_ym = {Y: yp}, {Y: ym}
    sib = {C: 1 - c}
    inner = {Z: 1 - l}
    outer = {Z: 1 - l, H: (h + 2 * l + 3) % 4}
    z = 2 * h + l
    zpeers = [{Z: (z + j) % 2, H: ((z + j) % 8) // 2} for j in range(1, 8)]
    hpeers = [{H: (h + j) % 4} for j in range(1, 4)]
    sems = Sems()
    sent = []

    def copy(src, dst, sem, to):
        return pltpu.make_async_remote_copy(
            src_ref=src,
            dst_ref=dst,
            send_sem=ss.at[sem],
            recv_sem=rs.at[sem],
            device_id=to,
            device_id_type=pl.DeviceIdType.MESH,
        )

    def send(src, dst, sem, to):
        made = copy(src, dst, sem, to)
        made.start()
        sent.append(made)

    def got(dst, sem):
        copy(dst, dst, sem, sib).wait_recv()

    mine = pl.ds(pl.multiple_of(l * TOK, TOK), TOK)
    theirs = pl.ds(pl.multiple_of((1 - l) * TOK, TOK), TOK)
    my_cols = pl.ds(pl.multiple_of(l * DH, 128), DH)
    their_cols = pl.ds(pl.multiple_of((1 - l) * DH, 128), DH)

    def slab_rows(xs, core, part=None):
        start = xs * SLAB + core * ROWS
        if part is None:
            return pl.ds(pl.multiple_of(start, 32), ROWS)
        return pl.ds(pl.multiple_of(start + part * HALF, 32), HALF)

    own_rows = slab_rows(x, c)
    loads = [
        pltpu.make_async_copy(dn_hbm, wd.at[own_rows, :], lsem.at[0]),
        pltpu.make_async_copy(gp_hbm, gpt.at[l], lsem.at[1]),
        pltpu.make_async_copy(up_hbm, upt.at[l], lsem.at[2]),
        pltpu.make_async_copy(gu_hbm, wg.at[own_rows, :], lsem.at[3]),
        pltpu.make_async_copy(g_hbm.at[:, my_cols], gb.at[mine, :], lsem.at[4]),
        pltpu.make_async_copy(a_hbm.at[:, my_cols], ab.at[mine, :], lsem.at[5]),
    ]
    for load in loads:
        load.start()

    barrier = pltpu.get_barrier_semaphore()
    greeted = [to_xp, to_xm, to_yp, to_ym, sib] + zpeers
    for peer in greeted:
        pl.semaphore_signal(barrier, inc=1, device_id=peer, device_id_type=pl.DeviceIdType.MESH)
    pl.semaphore_wait(barrier, len(greeted))

    class Weights:
        def __init__(self, ref):
            self.ref = ref
            self.plus = sems.block(3)
            self.minus = sems.block(3)
            self.side = sems.block(4)

        def put(self, rows, sem, to):
            send(self.ref.at[rows, :], self.ref.at[rows, :], sem, to)

        def open(self):
            self.put(slab_rows(x, c, 0), self.plus, to_xp)
            self.put(slab_rows(x, c, 1), self.minus, to_xm)
            self.put(slab_rows(x, c, 1), self.plus + 1, to_xp)
            self.put(slab_rows(x, c, 0), self.minus + 1, to_xm)
            self.put(own_rows, self.side, sib)

        def forward(self):
            got(self.ref.at[slab_rows(xm, c, 0), :], self.plus)
            self.put(slab_rows(xm, c, 0), self.plus + 2, to_xp)
            got(self.ref.at[slab_rows(xp, c, 1), :], self.minus)
            self.put(slab_rows(xp, c, 1), self.minus + 2, to_xm)

        def near(self):
            got(self.ref.at[slab_rows(xm, c, 1), :], self.plus + 1)
            self.put(slab_rows(xm, c), self.side + 1, sib)
            got(self.ref.at[slab_rows(xp, c, 0), :], self.minus + 1)
            self.put(slab_rows(xp, c), self.side + 2, sib)

        def far(self):
            got(self.ref.at[slab_rows(xo, c, 0), :], self.plus + 2)
            got(self.ref.at[slab_rows(xo, c, 1), :], self.minus + 2)
            self.put(slab_rows(xo, c), self.side + 3, sib)

        def side_got(self, k):
            got(self.ref.at[slab_rows((x, xm, xp, xo)[k], 1 - c), :], self.side + k)

    class Tokens:
        def __init__(self, ref):
            self.ref = ref
            self.over = sems.block(2)
            self.plus = sems.block(3)
            self.minus = sems.block(3)

        def at(self, group, quarter, part=None):
            start = group * TOK + quarter * QT
            if part is None:
                return self.ref.at[pl.ds(pl.multiple_of(start, 32), QT), :]
            return self.ref.at[pl.ds(pl.multiple_of(start + part * 32, 32), 32), :]

        def open(self, hbm, ways):
            for part, way in enumerate(ways):
                rows = pl.ds(pl.multiple_of(y * QT + part * 32, 32), 32)
                send(hbm.at[rows, their_cols], self.at(l, y, part), self.over + part, way)

        def spread(self):
            for part, (first, second) in enumerate(
                (((self.plus, to_yp), (self.minus + 1, to_ym)), ((self.minus, to_ym), (self.plus + 1, to_yp)))
            ):
                piece = self.at(1 - l, y, part)
                got(piece, self.over + part)
                send(piece, piece, *first)
                send(piece, piece, *second)

        def forward(self):
            piece = self.at(1 - l, ym, 0)
            got(piece, self.plus)
            send(piece, piece, self.plus + 2, to_yp)
            piece = self.at(1 - l, yp, 1)
            got(piece, self.minus)
            send(piece, piece, self.minus + 2, to_ym)

        def near_got(self):
            got(self.at(1 - l, ym, 1), self.plus + 1)
            got(self.at(1 - l, yp, 0), self.minus + 1)

        def far_got(self):
            got(self.at(1 - l, yo, 0), self.plus + 2)
            got(self.at(1 - l, yo, 1), self.minus + 2)

    down, gate_up = Weights(wd), Weights(wg)
    outs, acts = Tokens(gb), Tokens(ab)

    outs.open(g_hbm, (inner, outer))
    loads[0].wait()
    down.open()
    acts.open(a_hbm, (outer, outer))
    loads[1].wait()
    loads[2].wait()
    pre_sem = sems.block(2)
    send(gpt.at[l], gpt.at[l], pre_sem, inner)
    send(upt.at[l], upt.at[l], pre_sem + 1, inner)
    loads[3].wait()
    gate_up.open()

    outs.spread()
    down.forward()
    acts.spread()
    down.near()

    def factors(group, rows):
        gate = jnp.transpose(gpt[group].astype(F32))
        up = jnp.transpose(upt[group].astype(F32))
        sig = jax.nn.sigmoid(gate)
        silu = gate * sig
        silu_s[rows, :] = silu
        dgate_s[rows, :] = up * sig * (1.0 + gate * (1.0 - sig))
        hid[rows, :] = (silu * up).astype(BF)

    factors(l, mine)
    outs.forward()
    down.far()
    for k in range(4):
        down.side_got(k)
    loads[4].wait()

    part = jnp.dot(gb[mine, :], wd[...], preferred_element_type=F32)
    ghf[mine, :] = part
    ghs[mine, :] = part.astype(BF)
    own_sem = sems.block(1)
    send(ghs.at[mine, :], ghr.at[mine, :], own_sem, inner)

    gate_up.forward()
    acts.forward()
    got(gpt.at[1 - l], pre_sem)
    got(upt.at[1 - l], pre_sem + 1)
    factors(1 - l, theirs)

    quarter_sem = sems.block(4)
    quarters = (y, ym, yp, yo)

    def quarter_rows(group, k):
        return pl.ds(pl.multiple_of(group * TOK + quarters[k] * QT, QT), QT)

    for k in range(4):
        if k == 1:
            outs.near_got()
        if k == 3:
            outs.far_got()
        rows = quarter_rows(1 - l, k)
        part = jnp.dot(gb[rows, :], wd[...], preferred_element_type=F32)
        ghf[rows, :] = part
        ghs[rows, :] = part.astype(BF)
        send(ghs.at[rows, :], ghr.at[rows, :], quarter_sem + k, inner)

    gate_up.near()

    order = (xo, xp, xm, x)

    def own(core):
        return pl.ds(pl.multiple_of(core * ROWS, 32), ROWS)

    class Grad:
        def __init__(self, left, right, mat, recv, pair, near1, near2, out):
            self.left, self.right = left, right
            self.mat, self.recv, self.pair = mat, recv, pair
            self.near1, self.near2, self.out = near1, near2, out
            self.cross = sems.block(4)
            self.plus = sems.block(3)
            self.minus = sems.block(3)

        def multiply(self, k):
            xs = order[k]
            self.mat[k] = wgrad_slab(self.left, self.right, xs).astype(BF)
            send(self.mat.at[k, own(1 - c), :], self.recv.at[k], self.cross + k, sib)

        def pair_sum(self, k):
            got(self.recv.at[k], self.cross + k)
            return self.mat[k, own(c), :].astype(F32) + self.recv[k].astype(F32)

        def start(self):
            lo, hi = pl.ds(0, HALF), pl.ds(HALF, HALF)
            self.pair[0] = self.pair_sum(0).astype(BF)
            send(self.pair.at[0, lo, :], self.near1.at[0], self.plus, to_xp)
            send(self.pair.at[0, hi, :], self.near1.at[1], self.minus, to_xm)
            self.pair[1] = self.pair_sum(1).astype(BF)
            send(self.pair.at[1, hi, :], self.near2.at[0, hi, :], self.plus + 1, to_xp)
            self.pair[2] = self.pair_sum(2).astype(BF)
            send(self.pair.at[2, lo, :], self.near2.at[1, lo, :], self.minus + 1, to_xm)

        def relay(self):
            lo, hi = pl.ds(0, HALF), pl.ds(HALF, HALF)
            got(self.near1.at[0], self.plus)
            self.pair[1, lo, :] = (self.pair[1, lo, :].astype(F32) + self.near1[0].astype(F32)).astype(BF)
            send(self.pair.at[1, lo, :], self.near2.at[0, lo, :], self.plus + 2, to_xp)
            got(self.near1.at[1], self.minus)
            self.pair[2, hi, :] = (self.pair[2, hi, :].astype(F32) + self.near1[1].astype(F32)).astype(BF)
            send(self.pair.at[2, hi, :], self.near2.at[1, hi, :], self.minus + 2, to_xm)

        def finish(self):
            lo, hi = pl.ds(0, HALF), pl.ds(HALF, HALF)
            total = self.pair_sum(3)
            got(self.near2.at[0, hi, :], self.plus + 1)
            got(self.near2.at[0, lo, :], self.plus + 2)
            got(self.near2.at[1, lo, :], self.minus + 1)
            got(self.near2.at[1, hi, :], self.minus + 2)
            total = total + self.near2[0].astype(F32) + self.near2[1].astype(F32)
            self.out[...] = total * (1.0 / 16.0)

    grad_down = Grad(gb, hid, dws_d, dwr_d, vs_d, r1_d, r2_d, wd_out)
    grad_gate = Grad(ab, ghb, dws_g, dwr_g, vs_g, r1_g, r2_g, wg_out)

    for k in range(4):
        grad_down.multiply(k)
        if k == 1:
            gate_up.far()
        if k == 2:
            grad_down.start()

    def hidden_grads(rows):
        total = ghf[rows, :] + ghr[rows, :].astype(F32)
        ghb[rows, pl.ds(0, FD)] = (total * dgate_s[rows, :]).astype(BF)
        ghb[rows, pl.ds(FD, FD)] = (total * silu_s[rows, :]).astype(BF)

    got(ghr.at[theirs, :], own_sem)
    hidden_grads(theirs)
    for k in range(4):
        rows = quarter_rows(l, k)
        got(ghr.at[rows, :], quarter_sem + k)
        hidden_grads(rows)

    for k in range(4):
        gate_up.side_got(k)

    slabs = (x, xm, xp, xo)
    y_rs = [sems.block(6) for _ in range(4)]
    z_rs = [sems.block(7) for _ in range(4)]
    z_ag = [sems.block(3) for _ in range(4)]
    y_ag = [sems.block(6) for _ in range(4)]
    stores = []

    def add_to(ref, other):
        ref[...] = (ref[...].astype(F32) + other[...].astype(F32)).astype(BF)

    def stage0(q):
        rows = pl.ds(pl.multiple_of(slabs[q] * SLAB, 128), SLAB)
        prod = lax.dot_general(
            ghb[...], wg[rows, :], (((1,), (1,)), ((), ())), preferred_element_type=F32
        )
        pb[q] = prod.astype(BF).reshape(2, 4, QT, SLAB)
        s = y_rs[q]
        send(pb.at[q, 0, yo], r1p.at[q], s, to_yp)
        send(pb.at[q, 1, yo], r1m.at[q], s + 1, to_ym)
        send(pb.at[q, 1, yp], r2p.at[q, 1], s + 2, to_yp)
        send(pb.at[q, 0, ym], r2m.at[q, 0], s + 3, to_ym)

    def stage1(q):
        s = y_rs[q]
        got(r1p.at[q], s)
        add_to(pb.at[q, 0, yp], r1p.at[q])
        send(pb.at[q, 0, yp], r2p.at[q, 0], s + 4, to_yp)
        got(r1m.at[q], s + 1)
        add_to(pb.at[q, 1, ym], r1m.at[q])
        send(pb.at[q, 1, ym], r2m.at[q, 1], s + 5, to_ym)

    def stage2(q):
        s = y_rs[q]
        got(r2p.at[q, 1], s + 2)
        got(r2m.at[q, 0], s + 3)
        got(r2p.at[q, 0], s + 4)
        got(r2m.at[q, 1], s + 5)
        yb[q] = (
            pb[q, :, y].astype(F32) + r2p[q].astype(F32) + r2m[q].astype(F32)
        ).astype(BF)
        for j in range(1, 8):
            to = (z + j) % 8
            rows = pl.ds(pl.multiple_of((to // 2) * HT, HT), HT)
            send(yb.at[q, to % 2, rows, :], zr.at[q, j - 1], z_rs[q] + j - 1, zpeers[j - 1])

    def stage3(q):
        for j in range(7):
            got(zr.at[q, j], z_rs[q] + j)
        here = pl.ds(pl.multiple_of(h * HT, HT), HT)
        place = pl.ds(pl.multiple_of(y * QT + h * HT, HT), HT)
        same = yb[q, l, here, :].astype(F32)
        for j in (1, 3, 5):
            same = same + zr[q, j].astype(F32)
        other = zr[q, 0].astype(F32)
        for j in (2, 4, 6):
            other = other + zr[q, j].astype(F32)
        xs = slabs[q]
        ob[xs, l, place, :] = same.astype(BF)
        ob[xs, 1 - l, place, :] = other.astype(BF)
        for j in range(3):
            piece = ob.at[xs, :, place, :]
            send(piece, piece, z_ag[q] + j, hpeers[j])

    def quarter(q, half, which):
        return ob.at[slabs[q], half, pl.ds(pl.multiple_of(which * QT, QT), QT), :]

    def stage4(q):
        for j in range(3):
            rows = pl.ds(pl.multiple_of(y * QT + ((h + 3 - j) % 4) * HT, HT), HT)
            got(ob.at[slabs[q], :, rows, :], z_ag[q] + j)
        s = y_ag[q]
        send(quarter(q, 0, y), quarter(q, 0, y), s, to_yp)
        send(quarter(q, 1, y), quarter(q, 1, y), s + 1, to_ym)
        send(quarter(q, 1, y), quarter(q, 1, y), s + 2, to_yp)
        send(quarter(q, 0, y), quarter(q, 0, y), s + 3, to_ym)

    def stage5(q):
        s = y_ag[q]
        got(quarter(q, 0, ym), s)
        send(quarter(q, 0, ym), quarter(q, 0, ym), s + 4, to_yp)
        got(quarter(q, 1, yp), s + 1)
        send(quarter(q, 1, yp), quarter(q, 1, yp), s + 5, to_ym)

    def stage6(q):
        s = y_ag[q]
        got(quarter(q, 1, ym), s + 2)
        got(quarter(q, 0, yp), s + 3)
        got(quarter(q, 0, yo), s + 4)
        got(quarter(q, 1, yo), s + 5)
        for half in range(2):
            cols = pl.ds(pl.multiple_of(half * DH + slabs[q] * SLAB, 128), SLAB)
            store = pltpu.make_async_copy(ob.at[slabs[q], half], gi_hbm.at[:, cols], lsem.at[6 + 2 * q + half])
            store.start()
            stores.append(store)

    stages = (stage0, stage1, stage2, stage3, stage4, stage5, stage6)
    for tick in range(10):
        for s in range(6, -1, -1):
            if 0 <= tick - s < 4:
                stages[s](tick - s)
        if tick == 0:
            grad_down.relay()
            acts.near_got()
            acts.far_got()
            loads[5].wait()
            grad_gate.multiply(0)
            grad_gate.multiply(1)
        if tick == 1:
            grad_gate.multiply(2)
            grad_gate.start()
        if tick == 2:
            grad_gate.multiply(3)
        if tick == 4:
            grad_gate.relay()
        if tick == 5:
            grad_down.finish()
    grad_gate.finish()

    for store in stores:
        store.wait()
    for made in sent:
        made.wait_send()


def per_device(activations, grad_out, gate_pre, up_pre, gate_up, down_weight):
    joined = jnp.concatenate([gate_up[:, 0, :], gate_up[:, 1, :]], axis=1)
    hbm = pl.BlockSpec(memory_space=pl.ANY)
    vmem = pl.BlockSpec(memory_space=pltpu.VMEM)
    scratch = [
        pltpu.VMEM((2 * TOK, DH), BF),
        pltpu.VMEM((2 * TOK, DH), BF),
        pltpu.VMEM((DH, FD), BF),
        pltpu.VMEM((DH, FG), BF),
        pltpu.VMEM((2, FD, TOK), BF),
        pltpu.VMEM((2, FD, TOK), BF),
        pltpu.VMEM((2 * TOK, FD), F32),
        pltpu.VMEM((2 * TOK, FD), BF),
        pltpu.VMEM((2 * TOK, FD), BF),
        pltpu.VMEM((2 * TOK, FD), F32),
        pltpu.VMEM((2 * TOK, FD), F32),
        pltpu.VMEM((2 * TOK, FD), BF),
        pltpu.VMEM((2 * TOK, FG), BF),
        pltpu.VMEM((4, SLAB, FD), BF),
        pltpu.VMEM((4, ROWS, FD), BF),
        pltpu.VMEM((4, SLAB, FG), BF),
        pltpu.VMEM((4, ROWS, FG), BF),
        pltpu.VMEM((3, ROWS, FD), BF),
        pltpu.VMEM((3, ROWS, FG), BF),
        pltpu.VMEM((2, HALF, FD), BF),
        pltpu.VMEM((2, HALF, FG), BF),
        pltpu.VMEM((2, ROWS, FD), BF),
        pltpu.VMEM((2, ROWS, FG), BF),
        pltpu.VMEM((4, 2, 4, QT, SLAB), BF),
        pltpu.VMEM((4, QT, SLAB), BF),
        pltpu.VMEM((4, QT, SLAB), BF),
        pltpu.VMEM((4, 2, QT, SLAB), BF),
        pltpu.VMEM((4, 2, QT, SLAB), BF),
        pltpu.VMEM((4, 2, QT, SLAB), BF),
        pltpu.VMEM((4, 7, HT, SLAB), BF),
        pltpu.VMEM((4, 2, TOK, SLAB), BF),
        pltpu.SemaphoreType.DMA((14,)),
        pltpu.SemaphoreType.DMA((160,)),
        pltpu.SemaphoreType.DMA((160,)),
    ]
    grad_input, gate_grad, down_grad = pl.pallas_call(
        kernel,
        out_shape=(
            jax.ShapeDtypeStruct((TOK, D), BF),
            jax.ShapeDtypeStruct((ROWS, FG), F32),
            jax.ShapeDtypeStruct((ROWS, FD), F32),
        ),
        in_specs=[hbm] * 6,
        out_specs=(hbm, vmem, vmem),
        scratch_shapes=scratch,
        compiler_params=pltpu.CompilerParams(
            collective_id=0, has_side_effects=True, vmem_limit_bytes=63 * 1024 * 1024
        ),
    )(activations, grad_out, gate_pre.T, up_pre.T, joined, down_weight)
    return grad_input, gate_grad.reshape(ROWS, 2, FD), down_grad


def solution(mesh):
    split = Mesh(mesh.devices.reshape(2, 4, 2, 4, 4), (Z, X, C, H, Y))
    return jax.shard_map(
        per_device,
        mesh=split,
        in_specs=(
            P(DP, None),
            P(DP, None),
            P(DP, TENSOR),
            P(DP, TENSOR),
            P(DP, None, TENSOR),
            P(DP, TENSOR),
        ),
        out_specs=(P(DP, None), P(DP, None, TENSOR), P(DP, TENSOR)),
        check_vma=False,
    )
```

```python
import jax
import jax.numpy as jnp
from jax import lax
from jax.experimental import pallas as pl
from jax.experimental.pallas import tpu as pltpu
from jax.sharding import Mesh
from jax.sharding import PartitionSpec as P

Z, X, C, H, Y = "dp_0", "dp_1", "dp_2", "tensor_0", "tensor_1"
DP = (Z, X, C)
TENSOR = (H, Y)
BF = jnp.bfloat16
F32 = jnp.float32

TOK = 256
D = 5120
DH = D // 2
SLAB = 640
ROWS = 320
HALF = 160
FD = 448
FG = 896
QT = 64
HT = 16


class Sems:
    def __init__(self):
        self.n = 0

    def block(self, count=1):
        first = self.n
        self.n += count
        return first


def wgrad_slab(acts, right, xs):
    cols = pl.ds(pl.multiple_of(xs * SLAB, 128), SLAB)
    return lax.dot_general(
        acts[:, cols], right[...], (((0,), (0,)), ((), ())), preferred_element_type=F32
    )


def kernel(
    a_hbm,
    g_hbm,
    gp_hbm,
    up_hbm,
    gu_hbm,
    dn_hbm,
    ob,
    wg_out,
    wd_out,
    gu3,
    gb,
    ab,
    wd,
    wg,
    gpt,
    upt,
    ghf,
    ghs,
    ghr,
    silu_s,
    dgate_s,
    hid,
    ghb,
    dws_d,
    dwr_d,
    dws_g,
    dwr_g,
    vs_d,
    vs_g,
    r1_d,
    r1_g,
    r2_d,
    r2_g,
    pb,
    r1,
    r2,
    r3,
    yb,
    zr,
    lsem,
    ss,
    rs,
):
    l, x, c, h, y = (lax.axis_index(n) for n in (Z, X, C, H, Y))
    xp, xm, xo = (x + 1) % 4, (x + 3) % 4, (x + 2) % 4
    yp, ym, yo = (y + 1) % 4, (y + 3) % 4, (y + 2) % 4
    to_xp, to_xm = {X: xp}, {X: xm}
    to_yp, to_ym = {Y: yp}, {Y: ym}
    hp, hm, ho = (h + 1) % 4, (h + 3) % 4, (h + 2) % 4
    sib = {C: 1 - c}
    inner = {Z: 1 - l}
    outer = {Z: 1 - l, H: (h + 2 * l + 3) % 4}
    cross = [{Z: 1 - l, H: (h + j) % 4} for j in range(4)]
    along = [None] + [{H: (h + j) % 4} for j in range(1, 4)]
    sems = Sems()
    sent = []

    def copy(src, dst, sem, to):
        return pltpu.make_async_remote_copy(
            src_ref=src,
            dst_ref=dst,
            send_sem=ss.at[sem],
            recv_sem=rs.at[sem],
            device_id=to,
            device_id_type=pl.DeviceIdType.MESH,
        )

    def send(src, dst, sem, to):
        made = copy(src, dst, sem, to)
        made.start()
        sent.append(made)

    def got(dst, sem):
        copy(dst, dst, sem, sib).wait_recv()

    mine = pl.ds(pl.multiple_of(l * TOK, TOK), TOK)
    theirs = pl.ds(pl.multiple_of((1 - l) * TOK, TOK), TOK)
    my_cols = pl.ds(pl.multiple_of(l * DH, 128), DH)
    their_cols = pl.ds(pl.multiple_of((1 - l) * DH, 128), DH)

    def slab_rows(xs, core, part=None):
        start = xs * SLAB + core * ROWS
        if part is None:
            return pl.ds(pl.multiple_of(start, 32), ROWS)
        return pl.ds(pl.multiple_of(start + part * HALF, 32), HALF)

    own_rows = slab_rows(x, c)
    loads = [
        pltpu.make_async_copy(dn_hbm, wd.at[own_rows, :], lsem.at[0]),
        pltpu.make_async_copy(gp_hbm, gpt.at[l], lsem.at[1]),
        pltpu.make_async_copy(up_hbm, upt.at[l], lsem.at[2]),
        pltpu.make_async_copy(gu_hbm, gu3, lsem.at[3]),
        pltpu.make_async_copy(g_hbm.at[:, my_cols], gb.at[mine, :], lsem.at[4]),
        pltpu.make_async_copy(a_hbm.at[:, my_cols], ab.at[mine, :], lsem.at[5]),
    ]
    for load in loads:
        load.start()
    loads[3].wait()
    wg[own_rows, :] = gu3[...].reshape(ROWS, FG)

    barrier = pltpu.get_barrier_semaphore()
    greeted = [to_xp, to_xm, to_yp, to_ym, sib] + cross + along[1:]
    for peer in greeted:
        pl.semaphore_signal(barrier, inc=1, device_id=peer, device_id_type=pl.DeviceIdType.MESH)
    pl.semaphore_wait(barrier, len(greeted))

    class Weights:
        def __init__(self, ref):
            self.ref = ref
            self.plus = sems.block(3)
            self.minus = sems.block(3)
            self.side = sems.block(4)

        def put(self, rows, sem, to):
            send(self.ref.at[rows, :], self.ref.at[rows, :], sem, to)

        def open(self):
            self.put(slab_rows(x, c, 0), self.plus, to_xp)
            self.put(slab_rows(x, c, 1), self.minus, to_xm)
            self.put(slab_rows(x, c, 1), self.plus + 1, to_xp)
            self.put(slab_rows(x, c, 0), self.minus + 1, to_xm)
            self.put(own_rows, self.side, sib)

        def forward(self):
            got(self.ref.at[slab_rows(xm, c, 0), :], self.plus)
            self.put(slab_rows(xm, c, 0), self.plus + 2, to_xp)
            got(self.ref.at[slab_rows(xp, c, 1), :], self.minus)
            self.put(slab_rows(xp, c, 1), self.minus + 2, to_xm)

        def near(self):
            got(self.ref.at[slab_rows(xm, c, 1), :], self.plus + 1)
            self.put(slab_rows(xm, c), self.side + 1, sib)
            got(self.ref.at[slab_rows(xp, c, 0), :], self.minus + 1)
            self.put(slab_rows(xp, c), self.side + 2, sib)

        def far(self):
            got(self.ref.at[slab_rows(xo, c, 0), :], self.plus + 2)
            got(self.ref.at[slab_rows(xo, c, 1), :], self.minus + 2)
            self.put(slab_rows(xo, c), self.side + 3, sib)

        def side_got(self, k):
            got(self.ref.at[slab_rows((x, xm, xp, xo)[k], 1 - c), :], self.side + k)

    class Tokens:
        def __init__(self, ref):
            self.ref = ref
            self.over = sems.block(2)
            self.plus = sems.block(3)
            self.minus = sems.block(3)

        def at(self, group, quarter, part=None):
            start = group * TOK + quarter * QT
            if part is None:
                return self.ref.at[pl.ds(pl.multiple_of(start, 32), QT), :]
            return self.ref.at[pl.ds(pl.multiple_of(start + part * 32, 32), 32), :]

        def open(self, hbm, way):
            for part in range(2):
                rows = pl.ds(pl.multiple_of(y * QT + part * 32, 32), 32)
                send(hbm.at[rows, their_cols], self.at(l, y, part), self.over + part, way)

        def spread(self, part):
            piece = self.at(1 - l, y, part)
            got(piece, self.over + part)
            if part == 0:
                send(piece, piece, self.plus, to_yp)
                send(piece, piece, self.minus + 1, to_ym)
            else:
                send(piece, piece, self.minus, to_ym)
                send(piece, piece, self.plus + 1, to_yp)

        def forward(self, part):
            if part == 0:
                piece = self.at(1 - l, ym, 0)
                got(piece, self.plus)
                send(piece, piece, self.plus + 2, to_yp)
            else:
                piece = self.at(1 - l, yp, 1)
                got(piece, self.minus)
                send(piece, piece, self.minus + 2, to_ym)

        def near_got(self):
            got(self.at(1 - l, ym, 1), self.plus + 1)
            got(self.at(1 - l, yp, 0), self.minus + 1)

        def far_got(self):
            got(self.at(1 - l, yo, 0), self.plus + 2)
            got(self.at(1 - l, yo, 1), self.minus + 2)

    down, gate_up = Weights(wd), Weights(wg)
    outs = Tokens(gb)
    acts_sem = sems.block(2)
    pre_sem = sems.block(2)
    own_sem = sems.block(1)
    quarter_sem = sems.block(4)
    quarters = (y, ym, yp, yo)

    def acts_rows(part):
        first, count = ((0, 192), (192, 64))[part]
        return pl.ds(first, count), pl.ds(pl.multiple_of(l * TOK + first, 64), count), pl.ds(
            pl.multiple_of((1 - l) * TOK + first, 64), count
        )

    def acts_send(part, way):
        here, there, _ = acts_rows(part)
        send(a_hbm.at[here, their_cols], ab.at[there, :], acts_sem + part, way)

    def acts_got():
        for part in range(2):
            got(ab.at[acts_rows(part)[2], :], acts_sem + part)
        loads[5].wait()

    def pre_open():
        loads[1].wait()
        loads[2].wait()
        send(gpt.at[l], gpt.at[l], pre_sem, inner)
        send(upt.at[l], upt.at[l], pre_sem + 1, inner)

    def factors(group, rows):
        gate = jnp.transpose(gpt[group].astype(F32))
        up = jnp.transpose(upt[group].astype(F32))
        sig = jax.nn.sigmoid(gate)
        silu = gate * sig
        silu_s[rows, :] = silu
        dgate_s[rows, :] = up * sig * (1.0 + gate * (1.0 - sig))
        hid[rows, :] = (silu * up).astype(BF)

    def their_factors():
        got(gpt.at[1 - l], pre_sem)
        got(upt.at[1 - l], pre_sem + 1)
        factors(1 - l, theirs)

    def product(rows, sem):
        part = jnp.dot(gb[rows, :], wd[...], preferred_element_type=F32)
        ghf[rows, :] = part
        ghs[rows, :] = part.astype(BF)
        send(ghs.at[rows, :], ghr.at[rows, :], sem, inner)

    def own_product():
        for k in range(4):
            down.side_got(k)
        loads[4].wait()
        product(mine, own_sem)

    def quarter_rows(group, k):
        return pl.ds(pl.multiple_of(group * TOK + quarters[k] * QT, QT), QT)

    def quarter_product(k):
        product(quarter_rows(1 - l, k), quarter_sem + k)

    def near_products():
        outs.near_got()
        quarter_product(1)
        quarter_product(2)

    def far_product():
        outs.far_got()
        quarter_product(3)
        acts_send(1, inner)

    order = (xo, xp, xm, x)

    def own(core):
        return pl.ds(pl.multiple_of(core * ROWS, 32), ROWS)

    class Grad:
        def __init__(self, left, right, mat, recv, pair, near1, near2, out):
            self.left, self.right = left, right
            self.mat, self.recv, self.pair = mat, recv, pair
            self.near1, self.near2, self.out = near1, near2, out
            self.cross = sems.block(4)
            self.plus = sems.block(3)
            self.minus = sems.block(3)

        def multiply(self, k):
            xs = order[k]
            self.mat[k] = wgrad_slab(self.left, self.right, xs).astype(BF)
            send(self.mat.at[k, own(1 - c), :], self.recv.at[k], self.cross + k, sib)

        def pair_sum(self, k):
            got(self.recv.at[k], self.cross + k)
            return self.mat[k, own(c), :].astype(F32) + self.recv[k].astype(F32)

        def start(self):
            lo, hi = pl.ds(0, HALF), pl.ds(HALF, HALF)
            self.pair[0] = self.pair_sum(0).astype(BF)
            send(self.pair.at[0, lo, :], self.near1.at[0], self.plus, to_xp)
            send(self.pair.at[0, hi, :], self.near1.at[1], self.minus, to_xm)
            self.pair[1] = self.pair_sum(1).astype(BF)
            send(self.pair.at[1, hi, :], self.near2.at[0, hi, :], self.plus + 1, to_xp)
            self.pair[2] = self.pair_sum(2).astype(BF)
            send(self.pair.at[2, lo, :], self.near2.at[1, lo, :], self.minus + 1, to_xm)

        def relay(self):
            lo, hi = pl.ds(0, HALF), pl.ds(HALF, HALF)
            got(self.near1.at[0], self.plus)
            self.pair[1, lo, :] = (self.pair[1, lo, :].astype(F32) + self.near1[0].astype(F32)).astype(BF)
            send(self.pair.at[1, lo, :], self.near2.at[0, lo, :], self.plus + 2, to_xp)
            got(self.near1.at[1], self.minus)
            self.pair[2, hi, :] = (self.pair[2, hi, :].astype(F32) + self.near1[1].astype(F32)).astype(BF)
            send(self.pair.at[2, hi, :], self.near2.at[1, hi, :], self.minus + 2, to_xm)

        def finish(self):
            lo, hi = pl.ds(0, HALF), pl.ds(HALF, HALF)
            total = self.pair_sum(3)
            got(self.near2.at[0, hi, :], self.plus + 1)
            got(self.near2.at[0, lo, :], self.plus + 2)
            got(self.near2.at[1, lo, :], self.minus + 1)
            got(self.near2.at[1, hi, :], self.minus + 2)
            total = total + self.near2[0].astype(F32) + self.near2[1].astype(F32)
            total = total * (1.0 / 16.0)
            if self.out.ndim == 3:
                self.out[:, 0, :] = total[:, :FD]
                self.out[:, 1, :] = total[:, FD:]
            else:
                self.out[...] = total

    grad_down = Grad(gb, hid, dws_d, dwr_d, vs_d, r1_d, r2_d, wd_out)
    grad_gate = Grad(ab, ghb, dws_g, dwr_g, vs_g, r1_g, r2_g, wg_out)

    def hidden_grads(rows):
        total = ghf[rows, :] + ghr[rows, :].astype(F32)
        ghb[rows, pl.ds(0, FD)] = (total * dgate_s[rows, :]).astype(BF)
        ghb[rows, pl.ds(FD, FD)] = (total * silu_s[rows, :]).astype(BF)

    def their_grads():
        got(ghr.at[theirs, :], own_sem)
        hidden_grads(theirs)

    def my_grads():
        for k in range(4):
            got(ghr.at[quarter_rows(l, k), :], quarter_sem + k)
        hidden_grads(mine)

    slabs = (x, xm, xp, xo)
    y_rs = [sems.block(3) for _ in range(8)]
    z_rs = [sems.block(4) for _ in range(8)]
    z_ag = [sems.block(3) for _ in range(8)]
    y_ag = [sems.block(3) for _ in range(8)]

    def ways(i):
        if i % 2 == 0:
            return (to_yp, yp), (to_ym, ym)
        return (to_ym, ym), (to_yp, yp)

    def stage0(i):
        s, kind = i // 2, i % 2
        if kind == 0 and s > 0:
            gate_up.side_got(s)
        if i == 0:
            gate_up.side_got(0)
        rows = pl.ds(pl.multiple_of(slabs[s] * SLAB, 128), SLAB)
        prod = lax.dot_general(
            ghb[theirs if kind == 0 else mine, :],
            wg[rows, :],
            (((1,), (1,)), ((), ())),
            preferred_element_type=F32,
        )
        pb[i] = prod.astype(BF).reshape(4, QT, SLAB)
        (ahead, _), (behind, behind_y) = ways(i)
        send(pb.at[i, yo], r1.at[i], y_rs[i], ahead)
        send(pb.at[i, behind_y], r3.at[i], y_rs[i] + 1, behind)

    def stage1(i):
        (ahead, ahead_y), _ = ways(i)
        got(r1.at[i], y_rs[i])
        pb[i, ahead_y] = (pb[i, ahead_y].astype(F32) + r1[i].astype(F32)).astype(BF)
        send(pb.at[i, ahead_y], r2.at[i], y_rs[i] + 2, ahead)

    def stage2(i):
        got(r3.at[i], y_rs[i] + 1)
        got(r2.at[i], y_rs[i] + 2)
        yb[i] = (pb[i, y].astype(F32) + r2[i].astype(F32) + r3[i].astype(F32)).astype(BF)
        for j in (2, 1, 3, 0):
            to = cross[j] if i % 2 == 0 else along[j]
            if to is not None:
                rows = pl.ds(pl.multiple_of(((h + j) % 4) * HT, HT), HT)
                send(yb.at[i, rows, :], zr.at[i, j], z_rs[i] + j, to)

    def z_piece(i, which):
        half = 1 - l if i % 2 == 0 else l
        return ob.at[slabs[i // 2], half, pl.ds(pl.multiple_of(y * QT + which * HT, HT), HT), :]

    def stage3(i):
        if i % 2 == 0:
            got(zr.at[i, 0], z_rs[i])
            total = zr[i, 0].astype(F32)
        else:
            total = yb[i, pl.ds(pl.multiple_of(h * HT, HT), HT), :].astype(F32)
        for j in range(1, 4):
            got(zr.at[i, j], z_rs[i] + j)
            total = total + zr[i, j].astype(F32)
        piece = z_piece(i, h)
        piece[...] = total.astype(BF)
        send(piece, piece, z_ag[i], along[1])
        send(piece, piece, z_ag[i] + 1, along[3])

    def stage4(i):
        behind, to = (hm, along[1]) if i % 2 == 0 else (hp, along[3])
        piece = z_piece(i, behind)
        got(piece, z_ag[i] + i % 2)
        send(piece, piece, z_ag[i] + 2, to)

    def quarter(i, which):
        half = 1 - l if i % 2 == 0 else l
        return ob.at[slabs[i // 2], half, pl.ds(pl.multiple_of(which * QT, QT), QT), :]

    def stage5(i):
        got(z_piece(i, hp if i % 2 == 0 else hm), z_ag[i] + 1 - i % 2)
        got(z_piece(i, ho), z_ag[i] + 2)
        (ahead, _), (behind, _) = ways(i)
        send(quarter(i, y), quarter(i, y), y_ag[i], ahead)
        send(quarter(i, y), quarter(i, y), y_ag[i] + 1, behind)

    def stage6(i):
        (ahead, _), (_, behind_y) = ways(i)
        got(quarter(i, behind_y), y_ag[i])
        send(quarter(i, behind_y), quarter(i, behind_y), y_ag[i] + 2, ahead)

    def stage7(i):
        (_, ahead_y), _ = ways(i)
        got(quarter(i, ahead_y), y_ag[i] + 1)
        got(quarter(i, yo), y_ag[i] + 2)

    plan = []

    def at(time, fn, *args):
        plan.append((time, len(plan), fn, args))

    at(0.0, outs.open, g_hbm, outer)
    at(0.1, loads[0].wait)
    at(0.2, down.open)
    at(0.3, pre_open)
    at(0.4, acts_send, 0, outer)
    at(0.5, factors, l, mine)
    at(5.4, down.forward)
    at(5.5, gate_up.open)
    at(6.3, outs.spread, 0)
    at(8.9, down.near)
    at(9.8, outs.spread, 1)
    at(11.5, outs.forward, 0)
    at(11.6, their_factors)
    at(12.2, down.far)
    at(13.8, own_product)
    at(14.8, quarter_product, 0)
    at(15.0, outs.forward, 1)
    at(15.6, near_products)
    at(18.3, gate_up.forward)
    at(20.2, far_product)
    for k in range(4):
        at(20.5 + 0.1 * k, grad_down.multiply, k)
    at(21.2, their_grads)
    at(24.0, my_grads)
    at(24.8, gate_up.near)
    at(23.9, grad_down.start)
    at(31.0, gate_up.far)
    at(34.5, grad_down.relay)
    at(33.0, acts_got)
    for k in range(4):
        at(33.1 + 0.9 * k, grad_gate.multiply, k)
    at(37.0, grad_gate.start)
    at(47.0, grad_gate.relay)
    at(46.0, grad_down.finish)
    at(59.0, grad_gate.finish)
    first = (21.5, 24.5, 26.4, 28.8, 31.5, 34.1, 36.7, 39.4)
    for i in range(8):
        time = first[i]
        at(time, stage0, i)
        at(time + 3.0, stage1, i)
        at(time + 6.0, stage2, i)
        at(time + 12.0, stage3, i)
        at(time + 15.5, stage4, i)
        time = max(time + 19.0, 42.0 + 2.6 * i)
        at(time, stage5, i)
        at(time + 3.5, stage6, i)
        at(time + 8.0, stage7, i)
    for time, _, fn, args in sorted(plan, key=lambda step: step[:2]):
        with jax.named_scope(getattr(fn, "__name__", "step") + "_".join([""] + [str(v) for v in args if isinstance(v, int)])):
            fn(*args)

    with jax.named_scope("sends"):
        for made in sent:
            made.wait_send()


def finish(ob, wg, wd, gi_hbm, wg_hbm, wd_hbm, sem):
    copies = [pltpu.make_async_copy(wg, wg_hbm, sem.at[8]), pltpu.make_async_copy(wd, wd_hbm, sem.at[9])]
    for k in range(8):
        cols = pl.ds((k % 2) * DH + (k // 2) * SLAB, SLAB)
        copies.append(pltpu.make_async_copy(ob.at[k // 2, k % 2], gi_hbm.at[:, cols], sem.at[k]))
    for made in copies:
        made.start()
    for made in copies:
        made.wait()


def per_device(activations, grad_out, gate_pre, up_pre, gate_up, down_weight):
    hbm = pl.BlockSpec(memory_space=pl.ANY)
    vmem = pl.BlockSpec(memory_space=pltpu.VMEM)
    scratch = [
        pltpu.VMEM((ROWS, 2, FD), BF),
        pltpu.VMEM((2 * TOK, DH), BF),
        pltpu.VMEM((2 * TOK, DH), BF),
        pltpu.VMEM((DH, FD), BF),
        pltpu.VMEM((DH, FG), BF),
        pltpu.VMEM((2, FD, TOK), BF),
        pltpu.VMEM((2, FD, TOK), BF),
        pltpu.VMEM((2 * TOK, FD), F32),
        pltpu.VMEM((2 * TOK, FD), BF),
        pltpu.VMEM((2 * TOK, FD), BF),
        pltpu.VMEM((2 * TOK, FD), F32),
        pltpu.VMEM((2 * TOK, FD), F32),
        pltpu.VMEM((2 * TOK, FD), BF),
        pltpu.VMEM((2 * TOK, FG), BF),
        pltpu.VMEM((4, SLAB, FD), BF),
        pltpu.VMEM((4, ROWS, FD), BF),
        pltpu.VMEM((4, SLAB, FG), BF),
        pltpu.VMEM((4, ROWS, FG), BF),
        pltpu.VMEM((3, ROWS, FD), BF),
        pltpu.VMEM((3, ROWS, FG), BF),
        pltpu.VMEM((2, HALF, FD), BF),
        pltpu.VMEM((2, HALF, FG), BF),
        pltpu.VMEM((2, ROWS, FD), BF),
        pltpu.VMEM((2, ROWS, FG), BF),
        pltpu.VMEM((8, 4, QT, SLAB), BF),
        pltpu.VMEM((8, QT, SLAB), BF),
        pltpu.VMEM((8, QT, SLAB), BF),
        pltpu.VMEM((8, QT, SLAB), BF),
        pltpu.VMEM((8, QT, SLAB), BF),
        pltpu.VMEM((8, 4, HT, SLAB), BF),
        pltpu.SemaphoreType.DMA((6,)),
        pltpu.SemaphoreType.DMA((170,)),
        pltpu.SemaphoreType.DMA((170,)),
    ]
    held = pl.pallas_call(
        kernel,
        out_shape=(
            pltpu.VMEM((4, 2, TOK, SLAB), BF),
            pltpu.VMEM((ROWS, 2, FD), F32),
            pltpu.VMEM((ROWS, FD), F32),
        ),
        in_specs=[hbm] * 6,
        out_specs=(vmem, vmem, vmem),
        scratch_shapes=scratch,
        compiler_params=pltpu.CompilerParams(
            collective_id=0, has_side_effects=True, vmem_limit_bytes=56 * 1024 * 1024
        ),
        name="step",
    )(activations, grad_out, gate_pre.T, up_pre.T, gate_up, down_weight)
    held = [pltpu.with_memory_space_constraint(v, pltpu.VMEM) for v in held]
    return pl.pallas_call(
        finish,
        out_shape=(
            jax.ShapeDtypeStruct((TOK, D), BF),
            jax.ShapeDtypeStruct((ROWS, 2, FD), F32),
            jax.ShapeDtypeStruct((ROWS, FD), F32),
        ),
        in_specs=[vmem] * 3,
        out_specs=(hbm, hbm, hbm),
        scratch_shapes=[pltpu.SemaphoreType.DMA((10,))],
        compiler_params=pltpu.CompilerParams(vmem_limit_bytes=4 * 1024 * 1024),
        name="finish",
    )(*held)


def solution(mesh):
    split = Mesh(mesh.devices.reshape(2, 4, 2, 4, 4), (Z, X, C, H, Y))
    return jax.shard_map(
        per_device,
        mesh=split,
        in_specs=(
            P(DP, None),
            P(DP, None),
            P(DP, TENSOR),
            P(DP, TENSOR),
            P(DP, None, TENSOR),
            P(DP, TENSOR),
        ),
        out_specs=(P(DP, None), P(DP, None, TENSOR), P(DP, TENSOR)),
        check_vma=False,
    )
```

```python
import jax
import jax.numpy as jnp
from jax import lax
from jax.experimental import pallas as pl
from jax.experimental.pallas import tpu as pltpu
from jax.sharding import Mesh
from jax.sharding import PartitionSpec as P

Z, X, C, H, Y = "dp_0", "dp_1", "dp_2", "tensor_0", "tensor_1"
DP = (Z, X, C)
TENSOR = (H, Y)
BF = jnp.bfloat16
F32 = jnp.float32

TOK = 256
D = 5120
DH = D // 2
SLAB = 640
ROWS = 320
HALF = 160
FD = 448
FG = 896
QT = 64
HT = 16

CHUNKS = ((0, 0), (1, 0), (0, 1), (2, 0), (1, 1), (2, 1), (3, 0), (3, 1))
DIRECT_SUM = (0, 1, 7)
DIRECT_SPREAD = (0, 1, 6, 7)
ORDER = (
    "down.open", "outs.open", "pre_open", "down.forward", "spread_0", "down.near", "gate_up.open",
    "acts_send_0", "spread_1", "down.far", "own_product", "quarter_product_0", "forward_0", "forward_1",
    "their_factors", "gate_up.forward", "factors", "near_products", "far_product", "their_grads",
    "gate_up.near", "s0_0", "dmul_0", "s1_0", "dmul_1", "s0_1", "my_grads", "s1_1", "s0_2", "s0_3", "dmul_2",
    "s2_0", "s0_4", "gate_up.far", "grad_down.start", "s2_1", "gmul_0", "s1_2", "s0_5", "s3_0", "s1_3", "s3_1",
    "s1_4", "s0_6", "gmul_1", "s2_2", "s4_0", "s1_5", "grad_down.relay", "s0_7", "s2_3", "gmul_2", "s2_4",
    "s1_7", "s2_5", "s5_0", "dmul_3", "s3_3", "s1_6", "s4_1", "s5_1", "grad_gate.start", "s3_2", "s2_7", "s3_4",
    "s4_3", "s4_2", "s3_5", "s2_6", "s6_1", "s6_0", "s5_3", "s4_4", "s5_2", "s4_5", "s3_7", "s3_6", "s5_4",
    "s5_5", "s4_7", "gmul_3", "s5_7", "s4_6", "s5_6", "s6_3", "s6_2", "grad_gate.relay", "s6_4", "s6_5", "s6_6",
    "s6_7", "s7_0", "s7_2", "grad_gate.finish", "s7_5", "s7_4", "s7_3", "grad_down.finish", "s7_1", "s7_6",
    "s7_7",
)


class Sems:
    def __init__(self):
        self.n = 0

    def block(self, count=1):
        first = self.n
        self.n += count
        return first


def wgrad_slab(acts, right, xs):
    cols = pl.ds(pl.multiple_of(xs * SLAB, 128), SLAB)
    return lax.dot_general(
        acts[:, cols], right[...], (((0,), (0,)), ((), ())), preferred_element_type=F32
    )


def kernel(
    a_hbm,
    g_hbm,
    gp_hbm,
    up_hbm,
    gu_hbm,
    dn_hbm,
    ob,
    wg_out,
    wd_out,
    gu3,
    gb,
    ab,
    wd,
    wg,
    gpt,
    upt,
    ghf,
    ghs,
    ghr,
    silu_s,
    dgate_s,
    hid,
    ghb,
    dws_d,
    dwr_d,
    dws_g,
    dwr_g,
    vs_d,
    vs_g,
    r1_d,
    r1_g,
    r2_d,
    r2_g,
    pb,
    r1,
    r2,
    r3,
    yb,
    zr,
    lsem,
    ss,
    rs,
):
    l, x, c, h, y = (lax.axis_index(n) for n in (Z, X, C, H, Y))
    xp, xm, xo = (x + 1) % 4, (x + 3) % 4, (x + 2) % 4
    yp, ym, yo = (y + 1) % 4, (y + 3) % 4, (y + 2) % 4
    to_xp, to_xm = {X: xp}, {X: xm}
    to_yp, to_ym = {Y: yp}, {Y: ym}
    hp, hm, ho = (h + 1) % 4, (h + 3) % 4, (h + 2) % 4
    sib = {C: 1 - c}
    inner = {Z: 1 - l}
    outer = {Z: 1 - l, H: (h + 2 * l + 3) % 4}
    cross = [{Z: 1 - l, H: (h + j) % 4} for j in range(4)]
    along = [None] + [{H: (h + j) % 4} for j in range(1, 4)]
    sems = Sems()
    sent = []

    def copy(src, dst, sem, to):
        return pltpu.make_async_remote_copy(
            src_ref=src,
            dst_ref=dst,
            send_sem=ss.at[sem],
            recv_sem=rs.at[sem],
            device_id=to,
            device_id_type=pl.DeviceIdType.MESH,
        )

    def send(src, dst, sem, to):
        made = copy(src, dst, sem, to)
        made.start()
        sent.append(made)

    def got(dst, sem):
        copy(dst, dst, sem, sib).wait_recv()

    mine = pl.ds(pl.multiple_of(l * TOK, TOK), TOK)
    theirs = pl.ds(pl.multiple_of((1 - l) * TOK, TOK), TOK)
    my_cols = pl.ds(pl.multiple_of(l * DH, 128), DH)
    their_cols = pl.ds(pl.multiple_of((1 - l) * DH, 128), DH)

    def slab_rows(xs, core, part=None):
        start = xs * SLAB + core * ROWS
        if part is None:
            return pl.ds(pl.multiple_of(start, 32), ROWS)
        return pl.ds(pl.multiple_of(start + part * HALF, 32), HALF)

    own_rows = slab_rows(x, c)
    loads = [
        pltpu.make_async_copy(dn_hbm, wd.at[own_rows, :], lsem.at[0]),
        pltpu.make_async_copy(gp_hbm, gpt.at[l], lsem.at[1]),
        pltpu.make_async_copy(up_hbm, upt.at[l], lsem.at[2]),
        pltpu.make_async_copy(gu_hbm, gu3, lsem.at[3]),
        pltpu.make_async_copy(g_hbm.at[:, my_cols], gb.at[mine, :], lsem.at[4]),
        pltpu.make_async_copy(a_hbm.at[:, my_cols], ab.at[mine, :], lsem.at[5]),
    ]
    for load in loads:
        load.start()
    loads[3].wait()
    wg[own_rows, :] = gu3[...].reshape(ROWS, FG)

    barrier = pltpu.get_barrier_semaphore()
    greeted = [to_xp, to_xm, to_yp, to_ym, sib] + cross + along[1:]
    for peer in greeted:
        pl.semaphore_signal(barrier, inc=1, device_id=peer, device_id_type=pl.DeviceIdType.MESH)
    pl.semaphore_wait(barrier, len(greeted))

    class Weights:
        def __init__(self, ref):
            self.ref = ref
            self.plus = sems.block(3)
            self.minus = sems.block(3)
            self.side = sems.block(4)

        def put(self, rows, sem, to):
            send(self.ref.at[rows, :], self.ref.at[rows, :], sem, to)

        def open(self):
            self.put(slab_rows(x, c, 0), self.plus, to_xp)
            self.put(slab_rows(x, c, 1), self.minus, to_xm)
            self.put(slab_rows(x, c, 1), self.plus + 1, to_xp)
            self.put(slab_rows(x, c, 0), self.minus + 1, to_xm)
            self.put(own_rows, self.side, sib)

        def forward(self):
            got(self.ref.at[slab_rows(xm, c, 0), :], self.plus)
            self.put(slab_rows(xm, c, 0), self.plus + 2, to_xp)
            got(self.ref.at[slab_rows(xp, c, 1), :], self.minus)
            self.put(slab_rows(xp, c, 1), self.minus + 2, to_xm)

        def near(self):
            got(self.ref.at[slab_rows(xm, c, 1), :], self.plus + 1)
            self.put(slab_rows(xm, c), self.side + 1, sib)
            got(self.ref.at[slab_rows(xp, c, 0), :], self.minus + 1)
            self.put(slab_rows(xp, c), self.side + 2, sib)

        def far(self):
            got(self.ref.at[slab_rows(xo, c, 0), :], self.plus + 2)
            got(self.ref.at[slab_rows(xo, c, 1), :], self.minus + 2)
            self.put(slab_rows(xo, c), self.side + 3, sib)

        def side_got(self, k):
            got(self.ref.at[slab_rows((x, xm, xp, xo)[k], 1 - c), :], self.side + k)

    class Tokens:
        def __init__(self, ref):
            self.ref = ref
            self.over = sems.block(2)
            self.plus = sems.block(3)
            self.minus = sems.block(3)

        def at(self, group, quarter, part=None):
            start = group * TOK + quarter * QT
            if part is None:
                return self.ref.at[pl.ds(pl.multiple_of(start, 32), QT), :]
            return self.ref.at[pl.ds(pl.multiple_of(start + part * 32, 32), 32), :]

        def open(self, hbm, way):
            for part in range(2):
                rows = pl.ds(pl.multiple_of(y * QT + part * 32, 32), 32)
                send(hbm.at[rows, their_cols], self.at(l, y, part), self.over + part, way)

        def spread(self, part):
            piece = self.at(1 - l, y, part)
            got(piece, self.over + part)
            if part == 0:
                send(piece, piece, self.plus, to_yp)
                send(piece, piece, self.minus + 1, to_ym)
            else:
                send(piece, piece, self.minus, to_ym)
                send(piece, piece, self.plus + 1, to_yp)

        def forward(self, part):
            if part == 0:
                piece = self.at(1 - l, ym, 0)
                got(piece, self.plus)
                send(piece, piece, self.plus + 2, to_yp)
            else:
                piece = self.at(1 - l, yp, 1)
                got(piece, self.minus)
                send(piece, piece, self.minus + 2, to_ym)

        def near_got(self):
            got(self.at(1 - l, ym, 1), self.plus + 1)
            got(self.at(1 - l, yp, 0), self.minus + 1)

        def far_got(self):
            got(self.at(1 - l, yo, 0), self.plus + 2)
            got(self.at(1 - l, yo, 1), self.minus + 2)

    down, gate_up = Weights(wd), Weights(wg)
    outs = Tokens(gb)
    acts_sem = sems.block(2)
    pre_sem = sems.block(2)
    own_sem = sems.block(1)
    quarter_sem = sems.block(4)
    quarters = (y, ym, yp, yo)

    def acts_rows(part):
        first, count = ((0, 192), (192, 64))[part]
        return pl.ds(first, count), pl.ds(pl.multiple_of(l * TOK + first, 64), count), pl.ds(
            pl.multiple_of((1 - l) * TOK + first, 64), count
        )

    def acts_send(part, way):
        here, there, _ = acts_rows(part)
        send(a_hbm.at[here, their_cols], ab.at[there, :], acts_sem + part, way)

    def acts_got():
        for part in range(2):
            got(ab.at[acts_rows(part)[2], :], acts_sem + part)
        loads[5].wait()

    def pre_open():
        loads[1].wait()
        loads[2].wait()
        send(gpt.at[l], gpt.at[l], pre_sem, inner)
        send(upt.at[l], upt.at[l], pre_sem + 1, inner)
        acts_send(1, inner)

    def factors(group, rows):
        gate = jnp.transpose(gpt[group].astype(F32))
        up = jnp.transpose(upt[group].astype(F32))
        sig = jax.nn.sigmoid(gate)
        silu = gate * sig
        silu_s[rows, :] = silu
        dgate_s[rows, :] = up * sig * (1.0 + gate * (1.0 - sig))
        hid[rows, :] = (silu * up).astype(BF)

    def their_factors():
        got(gpt.at[1 - l], pre_sem)
        got(upt.at[1 - l], pre_sem + 1)
        factors(1 - l, theirs)

    def product(rows, sem):
        part = jnp.dot(gb[rows, :], wd[...], preferred_element_type=F32)
        ghf[rows, :] = part
        ghs[rows, :] = part.astype(BF)
        send(ghs.at[rows, :], ghr.at[rows, :], sem, inner)

    def own_product():
        for k in range(4):
            down.side_got(k)
        loads[4].wait()
        product(mine, own_sem)

    def quarter_rows(group, k):
        return pl.ds(pl.multiple_of(group * TOK + quarters[k] * QT, QT), QT)

    def quarter_product(k):
        product(quarter_rows(1 - l, k), quarter_sem + k)

    def near_products():
        outs.near_got()
        quarter_product(1)
        quarter_product(2)

    def far_product():
        outs.far_got()
        quarter_product(3)

    order = (xo, xp, xm, x)

    def own(core):
        return pl.ds(pl.multiple_of(core * ROWS, 32), ROWS)

    class Grad:
        def __init__(self, left, right, mat, recv, pair, near1, near2, out):
            self.left, self.right = left, right
            self.mat, self.recv, self.pair = mat, recv, pair
            self.near1, self.near2, self.out = near1, near2, out
            self.cross = sems.block(4)
            self.plus = sems.block(3)
            self.minus = sems.block(3)

        def multiply(self, k):
            xs = order[k]
            self.mat[k] = wgrad_slab(self.left, self.right, xs).astype(BF)
            send(self.mat.at[k, own(1 - c), :], self.recv.at[k], self.cross + k, sib)

        def pair_sum(self, k):
            got(self.recv.at[k], self.cross + k)
            return self.mat[k, own(c), :].astype(F32) + self.recv[k].astype(F32)

        def start(self):
            lo, hi = pl.ds(0, HALF), pl.ds(HALF, HALF)
            self.pair[0] = self.pair_sum(0).astype(BF)
            send(self.pair.at[0, lo, :], self.near1.at[0], self.plus, to_xp)
            send(self.pair.at[0, hi, :], self.near1.at[1], self.minus, to_xm)
            self.pair[1] = self.pair_sum(1).astype(BF)
            send(self.pair.at[1, hi, :], self.near2.at[0, hi, :], self.plus + 1, to_xp)
            self.pair[2] = self.pair_sum(2).astype(BF)
            send(self.pair.at[2, lo, :], self.near2.at[1, lo, :], self.minus + 1, to_xm)

        def relay(self):
            lo, hi = pl.ds(0, HALF), pl.ds(HALF, HALF)
            got(self.near1.at[0], self.plus)
            self.pair[1, lo, :] = (self.pair[1, lo, :].astype(F32) + self.near1[0].astype(F32)).astype(BF)
            send(self.pair.at[1, lo, :], self.near2.at[0, lo, :], self.plus + 2, to_xp)
            got(self.near1.at[1], self.minus)
            self.pair[2, hi, :] = (self.pair[2, hi, :].astype(F32) + self.near1[1].astype(F32)).astype(BF)
            send(self.pair.at[2, hi, :], self.near2.at[1, hi, :], self.minus + 2, to_xm)

        def finish(self):
            lo, hi = pl.ds(0, HALF), pl.ds(HALF, HALF)
            total = self.pair_sum(3)
            got(self.near2.at[0, hi, :], self.plus + 1)
            got(self.near2.at[0, lo, :], self.plus + 2)
            got(self.near2.at[1, lo, :], self.minus + 1)
            got(self.near2.at[1, hi, :], self.minus + 2)
            total = total + self.near2[0].astype(F32) + self.near2[1].astype(F32)
            total = total * (1.0 / 16.0)
            if self.out.ndim == 3:
                self.out[:, 0, :] = total[:, :FD]
                self.out[:, 1, :] = total[:, FD:]
            else:
                self.out[...] = total

    grad_down = Grad(gb, hid, dws_d, dwr_d, vs_d, r1_d, r2_d, wd_out)
    grad_gate = Grad(ab, ghb, dws_g, dwr_g, vs_g, r1_g, r2_g, wg_out)

    def hidden_grads(rows):
        total = ghf[rows, :] + ghr[rows, :].astype(F32)
        ghb[rows, pl.ds(0, FD)] = (total * dgate_s[rows, :]).astype(BF)
        ghb[rows, pl.ds(FD, FD)] = (total * silu_s[rows, :]).astype(BF)

    def their_grads():
        got(ghr.at[theirs, :], own_sem)
        hidden_grads(theirs)

    def my_grads():
        for k in range(4):
            got(ghr.at[quarter_rows(l, k), :], quarter_sem + k)
        hidden_grads(mine)

    slabs = [(x, xm, xp, xo)[k] for k, _ in CHUNKS]
    kinds = [kind for _, kind in CHUNKS]
    y_rs = [sems.block(3) for _ in range(8)]
    z_rs = [sems.block(4) for _ in range(8)]
    z_ag = [sems.block(3) for _ in range(8)]
    y_ag = [sems.block(3) for _ in range(8)]

    def ways(i):
        if i % 2 == 0:
            return (to_yp, yp), (to_ym, ym)
        return (to_ym, ym), (to_yp, yp)

    def stage0(i):
        k, kind = CHUNKS[i]
        if all(CHUNKS[e][0] != k for e in range(i)):
            gate_up.side_got(k)
        rows = pl.ds(pl.multiple_of(slabs[i] * SLAB, 128), SLAB)
        prod = lax.dot_general(
            ghb[theirs if kind == 0 else mine, :],
            wg[rows, :],
            (((1,), (1,)), ((), ())),
            preferred_element_type=F32,
        )
        pb[i] = prod.astype(BF).reshape(4, QT, SLAB)
        (ahead, ahead_y), (behind, behind_y) = ways(i)
        send(pb.at[i, yo], r1.at[i], y_rs[i], {Y: yo} if i in DIRECT_SUM else ahead)
        send(pb.at[i, behind_y], r3.at[i], y_rs[i] + 1, behind)
        if i in DIRECT_SUM:
            send(pb.at[i, ahead_y], r2.at[i], y_rs[i] + 2, ahead)

    def stage1(i):
        if i in DIRECT_SUM:
            return
        (ahead, ahead_y), _ = ways(i)
        got(r1.at[i], y_rs[i])
        pb[i, ahead_y] = (pb[i, ahead_y].astype(F32) + r1[i].astype(F32)).astype(BF)
        send(pb.at[i, ahead_y], r2.at[i], y_rs[i] + 2, ahead)

    def stage2(i):
        total = pb[i, y].astype(F32)
        if i in DIRECT_SUM:
            got(r1.at[i], y_rs[i])
            total = total + r1[i].astype(F32)
        got(r3.at[i], y_rs[i] + 1)
        got(r2.at[i], y_rs[i] + 2)
        yb[i] = (total + r2[i].astype(F32) + r3[i].astype(F32)).astype(BF)
        for j in (2, 1, 3, 0):
            to = cross[j] if kinds[i] == 0 else along[j]
            if to is not None:
                rows = pl.ds(pl.multiple_of(((h + j) % 4) * HT, HT), HT)
                send(yb.at[i, rows, :], zr.at[i, j], z_rs[i] + j, to)

    def piece_of(i, first, count):
        half = 1 - l if kinds[i] == 0 else l
        return ob.at[slabs[i], half, pl.ds(pl.multiple_of(first, HT), count), :]

    def z_piece(i, which):
        return piece_of(i, y * QT + which * HT, HT)

    def quarter(i, which):
        return piece_of(i, which * QT, QT)

    def stage3(i):
        if kinds[i] == 0:
            got(zr.at[i, 0], z_rs[i])
            total = zr[i, 0].astype(F32)
        else:
            total = yb[i, pl.ds(pl.multiple_of(h * HT, HT), HT), :].astype(F32)
        for j in range(1, 4):
            got(zr.at[i, j], z_rs[i] + j)
            total = total + zr[i, j].astype(F32)
        piece = z_piece(i, h)
        piece[...] = total.astype(BF)
        if i in DIRECT_SPREAD:
            send(piece, piece, z_ag[i] + 2, along[2])
        send(piece, piece, z_ag[i], along[1])
        send(piece, piece, z_ag[i] + 1, along[3])

    def stage4(i):
        if i in DIRECT_SPREAD:
            return
        behind, to = (hm, along[1]) if i % 2 == 0 else (hp, along[3])
        piece = z_piece(i, behind)
        got(piece, z_ag[i] + i % 2)
        send(piece, piece, z_ag[i] + 2, to)

    def stage5(i):
        if i in DIRECT_SPREAD:
            got(z_piece(i, hm), z_ag[i])
            got(z_piece(i, hp), z_ag[i] + 1)
        else:
            got(z_piece(i, hp if i % 2 == 0 else hm), z_ag[i] + 1 - i % 2)
        got(z_piece(i, ho), z_ag[i] + 2)
        (ahead, _), (behind, _) = ways(i)
        send(quarter(i, y), quarter(i, y), y_ag[i], ahead)
        send(quarter(i, y), quarter(i, y), y_ag[i] + 1, behind)

    def stage6(i):
        (ahead, _), (_, behind_y) = ways(i)
        got(quarter(i, behind_y), y_ag[i])
        send(quarter(i, behind_y), quarter(i, behind_y), y_ag[i] + 2, ahead)

    def stage7(i):
        (_, ahead_y), _ = ways(i)
        got(quarter(i, ahead_y), y_ag[i] + 1)
        got(quarter(i, yo), y_ag[i] + 2)

    steps = {
        "outs.open": lambda: outs.open(g_hbm, outer),
        "down.open": lambda: (loads[0].wait(), down.open()),
        "pre_open": pre_open,
        "acts_send_0": lambda: acts_send(0, outer),
        "factors": lambda: factors(l, mine),
        "down.forward": down.forward,
        "gate_up.open": gate_up.open,
        "down.near": down.near,
        "their_factors": their_factors,
        "down.far": down.far,
        "own_product": own_product,
        "quarter_product_0": lambda: quarter_product(0),
        "near_products": near_products,
        "gate_up.forward": gate_up.forward,
        "far_product": far_product,
        "gate_up.near": gate_up.near,
        "gate_up.far": gate_up.far,
        "their_grads": their_grads,
        "my_grads": my_grads,
        "grad_down.start": grad_down.start,
        "grad_down.relay": grad_down.relay,
        "grad_down.finish": grad_down.finish,
        "grad_gate.start": grad_gate.start,
        "grad_gate.relay": grad_gate.relay,
        "grad_gate.finish": grad_gate.finish,
        "dmul": grad_down.multiply,
        "gmul": lambda k: (acts_got() if k == 0 else None, grad_gate.multiply(k)),
        "spread": outs.spread,
        "forward": outs.forward,
    }
    for n, stage in enumerate((stage0, stage1, stage2, stage3, stage4, stage5, stage6, stage7)):
        steps[f"s{n}"] = stage
    for name in ORDER:
        with jax.named_scope(name):
            base, _, number = name.rpartition("_")
            if name in steps:
                steps[name]()
            else:
                steps[base](int(number))

    with jax.named_scope("sends"):
        for made in sent:
            made.wait_send()


def finish(ob, wg, wd, gi_hbm, wg_hbm, wd_hbm, sem):
    copies = [pltpu.make_async_copy(wg, wg_hbm, sem.at[8]), pltpu.make_async_copy(wd, wd_hbm, sem.at[9])]
    for k in range(8):
        cols = pl.ds((k % 2) * DH + (k // 2) * SLAB, SLAB)
        copies.append(pltpu.make_async_copy(ob.at[k // 2, k % 2], gi_hbm.at[:, cols], sem.at[k]))
    for made in copies:
        made.start()
    for made in copies:
        made.wait()


def per_device(activations, grad_out, gate_pre, up_pre, gate_up, down_weight):
    hbm = pl.BlockSpec(memory_space=pl.ANY)
    vmem = pl.BlockSpec(memory_space=pltpu.VMEM)
    scratch = [
        pltpu.VMEM((ROWS, 2, FD), BF),
        pltpu.VMEM((2 * TOK, DH), BF),
        pltpu.VMEM((2 * TOK, DH), BF),
        pltpu.VMEM((DH, FD), BF),
        pltpu.VMEM((DH, FG), BF),
        pltpu.VMEM((2, FD, TOK), BF),
        pltpu.VMEM((2, FD, TOK), BF),
        pltpu.VMEM((2 * TOK, FD), F32),
        pltpu.VMEM((2 * TOK, FD), BF),
        pltpu.VMEM((2 * TOK, FD), BF),
        pltpu.VMEM((2 * TOK, FD), F32),
        pltpu.VMEM((2 * TOK, FD), F32),
        pltpu.VMEM((2 * TOK, FD), BF),
        pltpu.VMEM((2 * TOK, FG), BF),
        pltpu.VMEM((4, SLAB, FD), BF),
        pltpu.VMEM((4, ROWS, FD), BF),
        pltpu.VMEM((4, SLAB, FG), BF),
        pltpu.VMEM((4, ROWS, FG), BF),
        pltpu.VMEM((3, ROWS, FD), BF),
        pltpu.VMEM((3, ROWS, FG), BF),
        pltpu.VMEM((2, HALF, FD), BF),
        pltpu.VMEM((2, HALF, FG), BF),
        pltpu.VMEM((2, ROWS, FD), BF),
        pltpu.VMEM((2, ROWS, FG), BF),
        pltpu.VMEM((8, 4, QT, SLAB), BF),
        pltpu.VMEM((8, QT, SLAB), BF),
        pltpu.VMEM((8, QT, SLAB), BF),
        pltpu.VMEM((8, QT, SLAB), BF),
        pltpu.VMEM((8, QT, SLAB), BF),
        pltpu.VMEM((8, 4, HT, SLAB), BF),
        pltpu.SemaphoreType.DMA((6,)),
        pltpu.SemaphoreType.DMA((170,)),
        pltpu.SemaphoreType.DMA((170,)),
    ]
    held = pl.pallas_call(
        kernel,
        out_shape=(
            pltpu.VMEM((4, 2, TOK, SLAB), BF),
            pltpu.VMEM((ROWS, 2, FD), F32),
            pltpu.VMEM((ROWS, FD), F32),
        ),
        in_specs=[hbm] * 6,
        out_specs=(vmem, vmem, vmem),
        scratch_shapes=scratch,
        compiler_params=pltpu.CompilerParams(
            collective_id=0, has_side_effects=True, vmem_limit_bytes=56 * 1024 * 1024
        ),
        name="step",
    )(activations, grad_out, gate_pre.T, up_pre.T, gate_up, down_weight)
    held = [pltpu.with_memory_space_constraint(v, pltpu.VMEM) for v in held]
    return pl.pallas_call(
        finish,
        out_shape=(
            jax.ShapeDtypeStruct((TOK, D), BF),
            jax.ShapeDtypeStruct((ROWS, 2, FD), F32),
            jax.ShapeDtypeStruct((ROWS, FD), F32),
        ),
        in_specs=[vmem] * 3,
        out_specs=(hbm, hbm, hbm),
        scratch_shapes=[pltpu.SemaphoreType.DMA((10,))],
        compiler_params=pltpu.CompilerParams(vmem_limit_bytes=4 * 1024 * 1024),
        name="finish",
    )(*held)


def solution(mesh):
    split = Mesh(mesh.devices.reshape(2, 4, 2, 4, 4), (Z, X, C, H, Y))
    return jax.shard_map(
        per_device,
        mesh=split,
        in_specs=(
            P(DP, None),
            P(DP, None),
            P(DP, TENSOR),
            P(DP, TENSOR),
            P(DP, None, TENSOR),
            P(DP, TENSOR),
        ),
        out_specs=(P(DP, None), P(DP, None, TENSOR), P(DP, TENSOR)),
        check_vma=False,
    )
```

```python
import jax
import jax.numpy as jnp
from jax import lax
from jax.experimental import pallas as pl
from jax.experimental.pallas import tpu as pltpu
from jax.sharding import Mesh
from jax.sharding import PartitionSpec as P

Z, X, C, H, Y = "dp_0", "dp_1", "dp_2", "tensor_0", "tensor_1"
DP = (Z, X, C)
TENSOR = (H, Y)
BF = jnp.bfloat16
F32 = jnp.float32

TOK = 256
D = 5120
DH = D // 2
SLAB = 640
ROWS = 320
HALF = 160
FD = 448
FG = 896
QT = 64
HT = 16

OUTLETS, INLETS = 12, 88
CHUNKS = ((0, 0), (1, 0), (2, 0), (0, 1), (1, 1), (2, 1), (3, 0), (3, 1))
DIRECT_SUM = (0, 1)
DIRECT_SPREAD = (0, 1, 5, 6, 7)
ORDER = (
    1, 2, 0, 3, 6, 60, 4, 7, 8, 61, 10, 70, 5, 11, 71, 13, 14, 9, 12, 15, 18, 100, 16, 40, 41, 42, 101, 102, 19,
    43, 20, 17, 103, 104, 120, 50, 121, 51, 112, 105, 21, 130, 113, 114, 131, 106, 122, 115, 52, 123, 107, 22,
    124, 23, 116, 151, 132, 125, 117, 150, 133, 142, 134, 126, 143, 127, 161, 152, 144, 160, 135, 24, 136, 153,
    154, 137, 171, 155, 53, 156, 162, 164, 170, 157, 163, 25, 165, 166, 167, 173, 174, 175, 172, 177, 176,
)


class Sems:
    def __init__(self):
        self.n = 0

    def block(self, count=1):
        first = self.n
        self.n += count
        return first


def wgrad_slab(acts, right, xs):
    cols = pl.ds(pl.multiple_of(xs * SLAB, 128), SLAB)
    return lax.dot_general(
        acts[:, cols], right[...], (((0,), (0,)), ((), ())), preferred_element_type=F32
    )


def kernel(
    a_hbm,
    g_hbm,
    gp_hbm,
    up_hbm,
    gu_hbm,
    dn_hbm,
    ob,
    wg_out,
    wd_out,
    gu3,
    gb,
    ab,
    wd,
    wg,
    gpt,
    upt,
    ghf,
    ghs,
    ghr,
    silu_s,
    dgate_s,
    hid,
    ghb,
    dws_d,
    dwr_d,
    dws_g,
    dwr_g,
    vs_d,
    vs_g,
    r1_d,
    r1_g,
    r2_d,
    r2_g,
    pb,
    r1,
    r2,
    r3,
    yb,
    zr,
    lsem,
    ss,
    rs,
):
    l, x, c, h, y = (lax.axis_index(n) for n in (Z, X, C, H, Y))
    xp, xm, xo = (x + 1) % 4, (x + 3) % 4, (x + 2) % 4
    yp, ym, yo = (y + 1) % 4, (y + 3) % 4, (y + 2) % 4
    to_xp, to_xm = {X: xp}, {X: xm}
    to_yp, to_ym = {Y: yp}, {Y: ym}
    hp, hm, ho = (h + 1) % 4, (h + 3) % 4, (h + 2) % 4
    sib = {C: 1 - c}
    inner = {Z: 1 - l}
    outer = {Z: 1 - l, H: (h + 2 * l + 3) % 4}
    cross = [{Z: 1 - l, H: (h + j) % 4} for j in range(4)]
    along = [None] + [{H: (h + j) % 4} for j in range(1, 4)]
    sems, outlets = Sems(), Sems()

    def copy(src, dst, outlet, sem, to):
        return pltpu.make_async_remote_copy(
            src_ref=src,
            dst_ref=dst,
            send_sem=ss.at[outlet],
            recv_sem=rs.at[sem],
            device_id=to,
            device_id_type=pl.DeviceIdType.MESH,
        )

    def send(src, dst, outlet, sem, to):
        copy(src, dst, outlet, sem, to).start()

    def got(like, sem):
        copy(like, like, 0, sem, sib).wait_recv()

    def gone(like, outlet):
        copy(like, like, outlet, 0, sib).wait_send()

    mine = pl.ds(pl.multiple_of(l * TOK, TOK), TOK)
    theirs = pl.ds(pl.multiple_of((1 - l) * TOK, TOK), TOK)
    my_cols = pl.ds(pl.multiple_of(l * DH, 128), DH)
    their_cols = pl.ds(pl.multiple_of((1 - l) * DH, 128), DH)

    def slab_rows(xs, core, part=None):
        start = xs * SLAB + core * ROWS
        if part is None:
            return pl.ds(pl.multiple_of(start, 32), ROWS)
        return pl.ds(pl.multiple_of(start + part * HALF, 32), HALF)

    barrier = pltpu.get_barrier_semaphore()
    greeted = [to_xp, to_xm, to_yp, to_ym, sib] + cross + along[1:]
    for peer in greeted:
        pl.semaphore_signal(barrier, inc=1, device_id=peer, device_id_type=pl.DeviceIdType.MESH)

    own_rows = slab_rows(x, c)
    loads = [
        pltpu.make_async_copy(dn_hbm, wd.at[own_rows, :], lsem.at[0]),
        pltpu.make_async_copy(gp_hbm, gpt.at[l], lsem.at[1]),
        pltpu.make_async_copy(up_hbm, upt.at[l], lsem.at[2]),
        pltpu.make_async_copy(gu_hbm, gu3, lsem.at[3]),
        pltpu.make_async_copy(g_hbm.at[:, my_cols], gb.at[mine, :], lsem.at[4]),
        pltpu.make_async_copy(a_hbm.at[:, my_cols], ab.at[mine, :], lsem.at[5]),
    ]
    for load in loads:
        load.start()
    pl.semaphore_wait(barrier, len(greeted))

    class Weights:
        def __init__(self, ref):
            self.ref = ref
            self.outlet = outlets.block()
            self.first, self.second, self.last = sems.block(), sems.block(), sems.block()
            self.side = [sems.block() for _ in range(4)]

        def put(self, rows, sem, to):
            send(self.ref.at[rows, :], self.ref.at[rows, :], self.outlet, sem, to)

        def open(self):
            self.put(slab_rows(x, c, 0), self.first, to_xp)
            self.put(slab_rows(x, c, 1), self.first, to_xm)
            self.put(slab_rows(x, c, 1), self.second, to_xp)
            self.put(slab_rows(x, c, 0), self.second, to_xm)
            self.put(own_rows, self.side[0], sib)

        def forward(self):
            got(self.ref.at[pl.ds(0, ROWS), :], self.first)
            self.put(slab_rows(xm, c, 0), self.last, to_xp)
            self.put(slab_rows(xp, c, 1), self.last, to_xm)

        def near(self):
            got(self.ref.at[pl.ds(0, ROWS), :], self.second)
            self.put(slab_rows(xm, c), self.side[1], sib)
            self.put(slab_rows(xp, c), self.side[2], sib)

        def far(self):
            got(self.ref.at[pl.ds(0, ROWS), :], self.last)
            self.put(slab_rows(xo, c), self.side[3], sib)

        def side_got(self, k):
            got(self.ref.at[pl.ds(0, ROWS), :], self.side[k])

        def drain(self):
            gone(self.ref.at[pl.ds(0, 7 * ROWS), :], self.outlet)

    class Tokens:
        def __init__(self, ref):
            self.ref = ref
            self.outlet = outlets.block()
            self.over = sems.block(2)
            self.plus, self.minus = sems.block(), sems.block()
            self.near, self.far = sems.block(), sems.block()

        def at(self, group, quarter, part=None):
            start = group * TOK + quarter * QT
            if part is None:
                return self.ref.at[pl.ds(pl.multiple_of(start, 32), QT), :]
            return self.ref.at[pl.ds(pl.multiple_of(start + part * 32, 32), 32), :]

        def open(self, hbm, way):
            for part in range(2):
                rows = pl.ds(pl.multiple_of(y * QT + part * 32, 32), 32)
                send(hbm.at[rows, their_cols], self.at(l, y, part), self.outlet, self.over + part, way)

        def put(self, piece, sem, to):
            send(piece, piece, self.outlet, sem, to)

        def spread(self, part):
            piece = self.at(1 - l, y, part)
            got(piece, self.over + part)
            if part == 0:
                self.put(piece, self.plus, to_yp)
                self.put(piece, self.near, to_ym)
            else:
                self.put(piece, self.minus, to_ym)
                self.put(piece, self.near, to_yp)

        def forward(self, part):
            piece = self.at(1 - l, (ym, yp)[part], part)
            got(piece, (self.plus, self.minus)[part])
            self.put(piece, self.far, (to_yp, to_ym)[part])

        def near_got(self):
            got(self.ref.at[pl.ds(0, QT), :], self.near)

        def far_got(self):
            got(self.ref.at[pl.ds(0, QT), :], self.far)

    down, gate_up = Weights(wd), Weights(wg)
    outs = Tokens(gb)
    acts_sem, pre_sem, own_sem, quarter_sem = (sems.block() for _ in range(4))
    acts_out, pre_out, product_out = (outlets.block() for _ in range(3))
    quarters = (y, ym, yp, yo)

    def acts_rows(part):
        first, count = ((0, 192), (192, 64))[part]
        return pl.ds(first, count), pl.ds(pl.multiple_of(l * TOK + first, 64), count)

    def acts_send(part, way):
        here, there = acts_rows(part)
        send(a_hbm.at[here, their_cols], ab.at[there, :], acts_out, acts_sem, way)

    def acts_got():
        got(ab.at[pl.ds(0, TOK), :], acts_sem)
        loads[5].wait()

    def pre_open():
        loads[1].wait()
        loads[2].wait()
        send(gpt.at[l], gpt.at[l], pre_out, pre_sem, inner)
        send(upt.at[l], upt.at[l], pre_out, pre_sem, inner)
        acts_send(1, inner)

    def own_gate_up():
        loads[3].wait()
        wg[own_rows, :] = gu3[...].reshape(ROWS, FG)

    def factors(group, rows):
        gate = jnp.transpose(gpt[group].astype(F32))
        up = jnp.transpose(upt[group].astype(F32))
        sig = jax.nn.sigmoid(gate)
        silu = gate * sig
        silu_s[rows, :] = silu
        dgate_s[rows, :] = up * sig * (1.0 + gate * (1.0 - sig))
        hid[rows, :] = (silu * up).astype(BF)

    def their_factors():
        got(gpt, pre_sem)
        factors(1 - l, theirs)

    def product(rows, part, sem):
        ghf[rows, :] = part
        ghs[rows, :] = part.astype(BF)
        send(ghs.at[rows, :], ghr.at[rows, :], product_out, sem, inner)

    def slab_product(xs):
        where = pl.ds(pl.multiple_of(xs * SLAB, 128), SLAB)
        return jnp.dot(gb[mine, where], wd[where, :], preferred_element_type=F32)

    def own_product():
        loads[4].wait()
        for k in range(3):
            down.side_got(k)
        part = slab_product(x) + slab_product(xm) + slab_product(xp)
        down.side_got(3)
        product(mine, part + slab_product(xo), own_sem)

    def quarter_rows(group, k):
        return pl.ds(pl.multiple_of(group * TOK + quarters[k] * QT, QT), QT)

    def quarter_product(k):
        rows = quarter_rows(1 - l, k)
        product(rows, jnp.dot(gb[rows, :], wd[...], preferred_element_type=F32), quarter_sem)

    def near_products():
        outs.near_got()
        quarter_product(1)
        quarter_product(2)

    def far_product():
        outs.far_got()
        quarter_product(3)

    order = (xo, xp, xm, x)

    def own(core):
        return pl.ds(pl.multiple_of(core * ROWS, 32), ROWS)

    class Grad:
        def __init__(self, left, right, mat, recv, pair, near1, near2, out):
            self.left, self.right = left, right
            self.mat, self.recv, self.pair = mat, recv, pair
            self.near1, self.near2, self.out = near1, near2, out
            self.like = wd if right is hid else wg
            self.outlet = outlets.block()
            self.early, self.late, self.first, self.rest = (sems.block() for _ in range(4))

        def got(self, rows, sem):
            got(self.like.at[pl.ds(0, rows), :], sem)

        def put(self, src, dst, sem, to):
            send(src, dst, self.outlet, sem, to)

        def drain(self):
            gone(self.like.at[pl.ds(0, 7 * ROWS), :], self.outlet)

        def multiply(self, k):
            xs = order[k]
            self.mat[k] = wgrad_slab(self.left, self.right, xs).astype(BF)
            self.put(self.mat.at[k, own(1 - c), :], self.recv.at[k], self.late if k == 3 else self.early, sib)

        def pair_sum(self, k):
            return self.mat[k, own(c), :].astype(F32) + self.recv[k].astype(F32)

        def start(self):
            lo, hi = pl.ds(0, HALF), pl.ds(HALF, HALF)
            self.got(3 * ROWS, self.early)
            self.pair[0] = self.pair_sum(0).astype(BF)
            self.put(self.pair.at[0, lo, :], self.near1.at[0], self.first, to_xp)
            self.put(self.pair.at[0, hi, :], self.near1.at[1], self.first, to_xm)
            self.pair[1] = self.pair_sum(1).astype(BF)
            self.put(self.pair.at[1, hi, :], self.near2.at[0, hi, :], self.rest, to_xp)
            self.pair[2] = self.pair_sum(2).astype(BF)
            self.put(self.pair.at[2, lo, :], self.near2.at[1, lo, :], self.rest, to_xm)

        def relay(self):
            lo, hi = pl.ds(0, HALF), pl.ds(HALF, HALF)
            self.got(ROWS, self.first)
            self.pair[1, lo, :] = (self.pair[1, lo, :].astype(F32) + self.near1[0].astype(F32)).astype(BF)
            self.put(self.pair.at[1, lo, :], self.near2.at[0, lo, :], self.rest, to_xp)
            self.pair[2, hi, :] = (self.pair[2, hi, :].astype(F32) + self.near1[1].astype(F32)).astype(BF)
            self.put(self.pair.at[2, hi, :], self.near2.at[1, hi, :], self.rest, to_xm)

        def finish(self):
            self.got(ROWS, self.late)
            total = self.pair_sum(3)
            self.got(2 * ROWS, self.rest)
            total = total + self.near2[0].astype(F32) + self.near2[1].astype(F32)
            total = total * (1.0 / 16.0)
            if self.out.ndim == 3:
                self.out[:, 0, :] = total[:, :FD]
                self.out[:, 1, :] = total[:, FD:]
            else:
                self.out[...] = total

    grad_down = Grad(gb, hid, dws_d, dwr_d, vs_d, r1_d, r2_d, wd_out)
    grad_gate = Grad(ab, ghb, dws_g, dwr_g, vs_g, r1_g, r2_g, wg_out)

    def hidden_grads(rows):
        total = ghf[rows, :] + ghr[rows, :].astype(F32)
        ghb[rows, pl.ds(0, FD)] = (total * dgate_s[rows, :]).astype(BF)
        ghb[rows, pl.ds(FD, FD)] = (total * silu_s[rows, :]).astype(BF)

    def their_grads():
        got(ghr.at[theirs, :], own_sem)
        hidden_grads(theirs)

    def my_grads():
        got(ghr.at[mine, :], quarter_sem)
        hidden_grads(mine)

    slabs = [(x, xm, xp, xo)[k] for k, _ in CHUNKS]
    kinds = [kind for _, kind in CHUNKS]
    y_sum = [(sems.block(), sems.block()) for _ in range(8)]
    z_sum = [sems.block() for _ in range(8)]
    z_all = [(sems.block(), sems.block()) for _ in range(8)]
    y_all = [(sems.block(), sems.block()) for _ in range(8)]
    y_sum_out, z_sum_out, z_all_out, y_all_out = (outlets.block() for _ in range(4))

    def ways(i):
        if i % 2 == 0:
            return (to_yp, yp), (to_ym, ym)
        return (to_ym, ym), (to_yp, yp)

    def stage0(i):
        k, kind = CHUNKS[i]
        if all(CHUNKS[e][0] != k for e in range(i)):
            gate_up.side_got(k)
        rows = pl.ds(pl.multiple_of(slabs[i] * SLAB, 128), SLAB)
        prod = lax.dot_general(
            ghb[theirs if kind == 0 else mine, :],
            wg[rows, :],
            (((1,), (1,)), ((), ())),
            preferred_element_type=F32,
        )
        pb[i] = prod.astype(BF).reshape(4, QT, SLAB)
        (ahead, ahead_y), (behind, behind_y) = ways(i)
        first, rest = y_sum[i]
        if i in DIRECT_SUM:
            send(pb.at[i, yo], r1.at[i], y_sum_out, rest, {Y: yo})
            send(pb.at[i, ahead_y], r2.at[i], y_sum_out, rest, ahead)
        else:
            send(pb.at[i, yo], r1.at[i], y_sum_out, first, ahead)
        send(pb.at[i, behind_y], r3.at[i], y_sum_out, rest, behind)

    def stage1(i):
        if i in DIRECT_SUM:
            return
        (ahead, ahead_y), _ = ways(i)
        first, rest = y_sum[i]
        got(r1.at[i], first)
        pb[i, ahead_y] = (pb[i, ahead_y].astype(F32) + r1[i].astype(F32)).astype(BF)
        send(pb.at[i, ahead_y], r2.at[i], y_sum_out, rest, ahead)

    def stage2(i):
        total = pb[i, y].astype(F32)
        got(pb.at[0, pl.ds(0, 3 if i in DIRECT_SUM else 2)], y_sum[i][1])
        if i in DIRECT_SUM:
            total = total + r1[i].astype(F32)
        yb[i] = (total + r2[i].astype(F32) + r3[i].astype(F32)).astype(BF)
        for j in (2, 1, 3, 0):
            to = cross[j] if kinds[i] == 0 else along[j]
            if to is not None:
                rows = pl.ds(pl.multiple_of(((h + j) % 4) * HT, HT), HT)
                send(yb.at[i, rows, :], zr.at[i, j], z_sum_out, z_sum[i], to)

    def piece_of(i, first, count):
        half = 1 - l if kinds[i] == 0 else l
        return ob.at[slabs[i], half, pl.ds(pl.multiple_of(first, HT), count), :]

    def z_piece(i, which):
        return piece_of(i, y * QT + which * HT, HT)

    def quarter(i, which):
        return piece_of(i, which * QT, QT)

    def stage3(i):
        if kinds[i] == 0:
            got(zr.at[i], z_sum[i])
            total = zr[i, 0].astype(F32)
        else:
            got(zr.at[i, pl.ds(1, 3)], z_sum[i])
            total = yb[i, pl.ds(pl.multiple_of(h * HT, HT), HT), :].astype(F32)
        for j in range(1, 4):
            total = total + zr[i, j].astype(F32)
        piece = z_piece(i, h)
        piece[...] = total.astype(BF)
        first, rest = z_all[i]
        if i in DIRECT_SPREAD:
            first = rest
            send(piece, piece, z_all_out, rest, along[2])
        turn = (first, rest) if i % 2 == 0 else (rest, first)
        send(piece, piece, z_all_out, turn[0], along[1])
        send(piece, piece, z_all_out, turn[1], along[3])

    def stage4(i):
        if i in DIRECT_SPREAD:
            return
        behind, to = (hm, along[1]) if i % 2 == 0 else (hp, along[3])
        first, rest = z_all[i]
        piece = z_piece(i, behind)
        got(piece, first)
        send(piece, piece, z_all_out, rest, to)

    def stage5(i):
        got(zr.at[0, pl.ds(0, 3 if i in DIRECT_SPREAD else 2)], z_all[i][1])
        (ahead, _), (behind, _) = ways(i)
        first, rest = y_all[i]
        send(quarter(i, y), quarter(i, y), y_all_out, first, ahead)
        send(quarter(i, y), quarter(i, y), y_all_out, rest, behind)

    def stage6(i):
        (ahead, _), (_, behind_y) = ways(i)
        first, rest = y_all[i]
        got(quarter(i, behind_y), first)
        send(quarter(i, behind_y), quarter(i, behind_y), y_all_out, rest, ahead)

    def stage7(i):
        got(pb.at[0, pl.ds(0, 2)], y_all[i][1])

    steps = (
        lambda: outs.open(g_hbm, outer),
        lambda: (loads[0].wait(), down.open()),
        pre_open,
        lambda: acts_send(0, outer),
        own_gate_up,
        lambda: factors(l, mine),
        down.forward,
        gate_up.open,
        down.near,
        their_factors,
        down.far,
        own_product,
        lambda: quarter_product(0),
        near_products,
        gate_up.forward,
        far_product,
        gate_up.near,
        gate_up.far,
        their_grads,
        my_grads,
        grad_down.start,
        grad_down.relay,
        grad_down.finish,
        grad_gate.start,
        grad_gate.relay,
        grad_gate.finish,
        grad_down.multiply,
        lambda k: (acts_got() if k == 0 else None, grad_gate.multiply(k)),
        outs.spread,
        outs.forward,
    )
    stages = (stage0, stage1, stage2, stage3, stage4, stage5, stage6, stage7)
    assert (outlets.n, sems.n) == (OUTLETS, INLETS), (outlets.n, sems.n)
    for code in ORDER:
        with jax.named_scope(f"{code}"):
            if code >= 100:
                stages[code // 10 - 10](code % 10)
            elif code >= 40:
                steps[code // 10 + 22](code % 10)
            else:
                steps[code]()

    with jax.named_scope("sends"):
        for part in (down, gate_up, grad_down, grad_gate):
            part.drain()
        gone(gb.at[pl.ds(0, TOK), :], outs.outlet)
        gone(ab.at[pl.ds(0, TOK), :], acts_out)
        gone(gpt, pre_out)
        gone(ghs, product_out)
        gone(pb.at[pl.ds(0, 6)], y_sum_out)
        gone(pb.at[pl.ds(0, 6)], y_all_out)
        gone(zr.at[pl.ds(0, 7)], z_sum_out)
        gone(zr.at[pl.ds(0, 6)], z_all_out)


def finish(ob, wg, wd, gi_hbm, wg_hbm, wd_hbm, sem):
    copies = [pltpu.make_async_copy(wg, wg_hbm, sem.at[8]), pltpu.make_async_copy(wd, wd_hbm, sem.at[9])]
    for k in range(8):
        cols = pl.ds((k % 2) * DH + (k // 2) * SLAB, SLAB)
        copies.append(pltpu.make_async_copy(ob.at[k // 2, k % 2], gi_hbm.at[:, cols], sem.at[k]))
    for made in copies:
        made.start()
    for made in copies:
        made.wait()


def per_device(activations, grad_out, gate_pre, up_pre, gate_up, down_weight):
    hbm = pl.BlockSpec(memory_space=pl.ANY)
    vmem = pl.BlockSpec(memory_space=pltpu.VMEM)
    scratch = [
        pltpu.VMEM((ROWS, 2, FD), BF),
        pltpu.VMEM((2 * TOK, DH), BF),
        pltpu.VMEM((2 * TOK, DH), BF),
        pltpu.VMEM((DH, FD), BF),
        pltpu.VMEM((DH, FG), BF),
        pltpu.VMEM((2, FD, TOK), BF),
        pltpu.VMEM((2, FD, TOK), BF),
        pltpu.VMEM((2 * TOK, FD), F32),
        pltpu.VMEM((2 * TOK, FD), BF),
        pltpu.VMEM((2 * TOK, FD), BF),
        pltpu.VMEM((2 * TOK, FD), F32),
        pltpu.VMEM((2 * TOK, FD), F32),
        pltpu.VMEM((2 * TOK, FD), BF),
        pltpu.VMEM((2 * TOK, FG), BF),
        pltpu.VMEM((4, SLAB, FD), BF),
        pltpu.VMEM((4, ROWS, FD), BF),
        pltpu.VMEM((4, SLAB, FG), BF),
        pltpu.VMEM((4, ROWS, FG), BF),
        pltpu.VMEM((3, ROWS, FD), BF),
        pltpu.VMEM((3, ROWS, FG), BF),
        pltpu.VMEM((2, HALF, FD), BF),
        pltpu.VMEM((2, HALF, FG), BF),
        pltpu.VMEM((2, ROWS, FD), BF),
        pltpu.VMEM((2, ROWS, FG), BF),
        pltpu.VMEM((8, 4, QT, SLAB), BF),
        pltpu.VMEM((8, QT, SLAB), BF),
        pltpu.VMEM((8, QT, SLAB), BF),
        pltpu.VMEM((8, QT, SLAB), BF),
        pltpu.VMEM((8, QT, SLAB), BF),
        pltpu.VMEM((8, 4, HT, SLAB), BF),
        pltpu.SemaphoreType.DMA((6,)),
        pltpu.SemaphoreType.DMA((OUTLETS,)),
        pltpu.SemaphoreType.DMA((INLETS,)),
    ]
    held = pl.pallas_call(
        kernel,
        out_shape=(
            pltpu.VMEM((4, 2, TOK, SLAB), BF),
            pltpu.VMEM((ROWS, 2, FD), F32),
            pltpu.VMEM((ROWS, FD), F32),
        ),
        in_specs=[hbm] * 6,
        out_specs=(vmem, vmem, vmem),
        scratch_shapes=scratch,
        compiler_params=pltpu.CompilerParams(
            collective_id=0, has_side_effects=True, vmem_limit_bytes=56 * 1024 * 1024
        ),
        name="step",
    )(activations, grad_out, gate_pre.T, up_pre.T, gate_up, down_weight)
    held = [pltpu.with_memory_space_constraint(v, pltpu.VMEM) for v in held]
    return pl.pallas_call(
        finish,
        out_shape=(
            jax.ShapeDtypeStruct((TOK, D), BF),
            jax.ShapeDtypeStruct((ROWS, 2, FD), F32),
            jax.ShapeDtypeStruct((ROWS, FD), F32),
        ),
        in_specs=[vmem] * 3,
        out_specs=(hbm, hbm, hbm),
        scratch_shapes=[pltpu.SemaphoreType.DMA((10,))],
        compiler_params=pltpu.CompilerParams(vmem_limit_bytes=4 * 1024 * 1024),
        name="finish",
    )(*held)


def solution(mesh):
    split = Mesh(mesh.devices.reshape(2, 4, 2, 4, 4), (Z, X, C, H, Y))
    return jax.shard_map(
        per_device,
        mesh=split,
        in_specs=(
            P(DP, None),
            P(DP, None),
            P(DP, TENSOR),
            P(DP, TENSOR),
            P(DP, None, TENSOR),
            P(DP, TENSOR),
        ),
        out_specs=(P(DP, None), P(DP, None, TENSOR), P(DP, TENSOR)),
        check_vma=False,
    )
```

```python
import jax
import jax.numpy as jnp
from jax import lax
from jax.experimental import pallas as pl
from jax.experimental.pallas import tpu as pltpu
from jax.sharding import Mesh
from jax.sharding import PartitionSpec as P

Z, X, C, H, Y = "dp_0", "dp_1", "dp_2", "tensor_0", "tensor_1"
DP = (Z, X, C)
TENSOR = (H, Y)
BF = jnp.bfloat16
F32 = jnp.float32

TOK = 256
D = 5120
DH = D // 2
SLAB = 640
ROWS = 320
HALF = 160
FD = 448
FG = 896
QT = 64
HT = 16

OUTLETS, INLETS = 12, 88
CHUNKS = ((0, 0), (1, 0), (2, 0), (0, 1), (1, 1), (2, 1), (3, 0), (3, 1))
DIRECT_SUM = (0, 1)
DIRECT_SPREAD = (0, 1, 5, 6, 7)
ORDER = (
    1, 2, 0, 3, 6, 60, 4, 7, 8, 61, 10, 70, 5, 11, 71, 13, 14, 9, 12, 15, 18, 100, 16, 40, 41, 42, 101, 102, 19,
    43, 20, 17, 103, 104, 120, 50, 121, 51, 112, 105, 21, 130, 113, 114, 131, 106, 122, 115, 52, 123, 107, 22,
    124, 23, 116, 151, 132, 125, 117, 150, 133, 142, 134, 126, 143, 127, 161, 152, 144, 160, 135, 24, 136, 153,
    154, 137, 171, 155, 53, 156, 162, 164, 170, 157, 163, 25, 165, 166, 167, 173, 174, 175, 172, 177, 176,
)


def pack(ref, first, value):
    n = value.shape[0]
    value = value.astype(BF)
    for tile in range(3):
        ref[pl.ds(first + tile * n, n), :] = value[:, tile * 128 : (tile + 1) * 128]
    tail = value[:, 384:]
    ref[pl.ds(first + 3 * n, n // 2), :] = jnp.concatenate([tail[: n // 2], tail[n // 2 :]], axis=1)


def unpack(ref, first, n):
    tiles = [ref[pl.ds(first + tile * n, n), :] for tile in range(3)]
    tail = ref[pl.ds(first + 3 * n, n // 2), :]
    return jnp.concatenate(tiles + [jnp.concatenate([tail[:, :64], tail[:, 64:]], axis=0)], axis=1)


class Sems:
    def __init__(self):
        self.n = 0

    def block(self, count=1):
        first = self.n
        self.n += count
        return first


def wgrad_slab(acts, right, xs):
    cols = pl.ds(pl.multiple_of(xs * SLAB, 128), SLAB)
    return lax.dot_general(
        acts[:, cols], right[...], (((0,), (0,)), ((), ())), preferred_element_type=F32
    )


def kernel(
    a_hbm,
    g_hbm,
    gp_hbm,
    up_hbm,
    gu_hbm,
    dn_hbm,
    ob,
    wg_out,
    wd_out,
    gu3,
    dnb,
    wp,
    gb,
    ab,
    wd,
    wg,
    gpt,
    upt,
    ghf,
    ghs,
    ghr,
    silu_s,
    dgate_s,
    hid,
    ghb,
    dws_d,
    dwr_d,
    dws_g,
    dwr_g,
    vs_d,
    vs_g,
    r1_d,
    r1_g,
    r2_d,
    r2_g,
    pb,
    r1,
    r2,
    r3,
    yb,
    zr,
    lsem,
    ss,
    rs,
):
    l, x, c, h, y = (lax.axis_index(n) for n in (Z, X, C, H, Y))
    xp, xm, xo = (x + 1) % 4, (x + 3) % 4, (x + 2) % 4
    yp, ym, yo = (y + 1) % 4, (y + 3) % 4, (y + 2) % 4
    to_xp, to_xm = {X: xp}, {X: xm}
    to_yp, to_ym = {Y: yp}, {Y: ym}
    hp, hm, ho = (h + 1) % 4, (h + 3) % 4, (h + 2) % 4
    sib = {C: 1 - c}
    inner = {Z: 1 - l}
    outer = {Z: 1 - l, H: (h + 2 * l + 3) % 4}
    cross = [{Z: 1 - l, H: (h + j) % 4} for j in range(4)]
    along = [None] + [{H: (h + j) % 4} for j in range(1, 4)]
    sems, outlets = Sems(), Sems()

    def copy(src, dst, outlet, sem, to):
        return pltpu.make_async_remote_copy(
            src_ref=src,
            dst_ref=dst,
            send_sem=ss.at[outlet],
            recv_sem=rs.at[sem],
            device_id=to,
            device_id_type=pl.DeviceIdType.MESH,
        )

    def send(src, dst, outlet, sem, to):
        copy(src, dst, outlet, sem, to).start()

    def got(like, sem):
        copy(like, like, 0, sem, sib).wait_recv()

    def gone(like, outlet):
        copy(like, like, outlet, 0, sib).wait_send()

    mine = pl.ds(pl.multiple_of(l * TOK, TOK), TOK)
    theirs = pl.ds(pl.multiple_of((1 - l) * TOK, TOK), TOK)
    my_cols = pl.ds(pl.multiple_of(l * DH, 128), DH)
    their_cols = pl.ds(pl.multiple_of((1 - l) * DH, 128), DH)

    def slab_rows(xs, core, part=None):
        start = xs * SLAB + core * ROWS
        if part is None:
            return pl.ds(pl.multiple_of(start, 32), ROWS)
        return pl.ds(pl.multiple_of(start + part * HALF, 32), HALF)

    barrier = pltpu.get_barrier_semaphore()
    greeted = [to_xp, to_xm, to_yp, to_ym, sib] + cross + along[1:]
    for peer in greeted:
        pl.semaphore_signal(barrier, inc=1, device_id=peer, device_id_type=pl.DeviceIdType.MESH)

    own_rows = slab_rows(x, c)
    loads = [
        pltpu.make_async_copy(dn_hbm, dnb, lsem.at[0]),
        pltpu.make_async_copy(gp_hbm, gpt.at[l], lsem.at[1]),
        pltpu.make_async_copy(up_hbm, upt.at[l], lsem.at[2]),
        pltpu.make_async_copy(gu_hbm, gu3, lsem.at[3]),
        pltpu.make_async_copy(g_hbm.at[:, my_cols], gb.at[mine, :], lsem.at[4]),
        pltpu.make_async_copy(a_hbm.at[:, my_cols], ab.at[mine, :], lsem.at[5]),
    ]
    for load in loads:
        load.start()
    loads[0].wait()
    for part in range(2):
        pack(wp.at[4 * x + 2 * c + part], 0, dnb[pl.ds(part * HALF, HALF), :])
    wd[own_rows, :] = dnb[...]
    pl.semaphore_wait(barrier, len(greeted))

    class Weights:
        def __init__(self, ref):
            self.ref = ref
            self.outlet = outlets.block()
            self.first, self.second, self.last = sems.block(), sems.block(), sems.block()
            self.side = [sems.block() for _ in range(4)]

        def block(self, xs, core, part=None):
            return self.ref.at[slab_rows(xs, core, part), :]

        def like(self, halves):
            return self.ref.at[pl.ds(0, halves * HALF), :]

        def ready(self, xs, core):
            pass

        def put(self, block, sem, to):
            send(block, block, self.outlet, sem, to)

        def open(self):
            self.put(self.block(x, c, 0), self.first, to_xp)
            self.put(self.block(x, c, 1), self.first, to_xm)
            self.put(self.block(x, c, 1), self.second, to_xp)
            self.put(self.block(x, c, 0), self.second, to_xm)
            self.put(self.block(x, c), self.side[0], sib)

        def forward(self):
            got(self.like(2), self.first)
            self.put(self.block(xm, c, 0), self.last, to_xp)
            self.put(self.block(xp, c, 1), self.last, to_xm)

        def near(self):
            got(self.like(2), self.second)
            self.put(self.block(xm, c), self.side[1], sib)
            self.put(self.block(xp, c), self.side[2], sib)
            self.ready(xm, c)
            self.ready(xp, c)

        def far(self):
            got(self.like(2), self.last)
            self.put(self.block(xo, c), self.side[3], sib)
            self.ready(xo, c)

        def side_got(self, k):
            got(self.like(2), self.side[k])
            self.ready((x, xm, xp, xo)[k], 1 - c)

        def drain(self):
            gone(self.like(14), self.outlet)

    class Packed(Weights):
        def block(self, xs, core, part=None):
            first = 4 * xs + 2 * core
            return wp.at[pl.ds(first, 2)] if part is None else wp.at[first + part]

        def like(self, halves):
            return wp.at[pl.ds(0, halves)]

        def ready(self, xs, core):
            for part in range(2):
                self.ref[slab_rows(xs, core, part), :] = unpack(self.block(xs, core, part), 0, HALF)

    class Tokens:
        def __init__(self, ref):
            self.ref = ref
            self.outlet = outlets.block()
            self.over = sems.block(2)
            self.plus, self.minus = sems.block(), sems.block()
            self.near, self.far = sems.block(), sems.block()

        def at(self, group, quarter, part=None):
            start = group * TOK + quarter * QT
            if part is None:
                return self.ref.at[pl.ds(pl.multiple_of(start, 32), QT), :]
            return self.ref.at[pl.ds(pl.multiple_of(start + part * 32, 32), 32), :]

        def open(self, hbm, way):
            for part in range(2):
                rows = pl.ds(pl.multiple_of(y * QT + part * 32, 32), 32)
                send(hbm.at[rows, their_cols], self.at(l, y, part), self.outlet, self.over + part, way)

        def put(self, piece, sem, to):
            send(piece, piece, self.outlet, sem, to)

        def spread(self, part):
            piece = self.at(1 - l, y, part)
            got(piece, self.over + part)
            if part == 0:
                self.put(piece, self.plus, to_yp)
                self.put(piece, self.near, to_ym)
            else:
                self.put(piece, self.minus, to_ym)
                self.put(piece, self.near, to_yp)

        def forward(self, part):
            piece = self.at(1 - l, (ym, yp)[part], part)
            got(piece, (self.plus, self.minus)[part])
            self.put(piece, self.far, (to_yp, to_ym)[part])

        def near_got(self):
            got(self.ref.at[pl.ds(0, QT), :], self.near)

        def far_got(self):
            got(self.ref.at[pl.ds(0, QT), :], self.far)

    down, gate_up = Packed(wd), Weights(wg)
    outs = Tokens(gb)
    acts_sem, pre_sem, own_sem, quarter_sem = (sems.block() for _ in range(4))
    acts_out, pre_out, product_out = (outlets.block() for _ in range(3))
    quarters = (y, ym, yp, yo)

    def acts_rows(part):
        first, count = ((0, 192), (192, 64))[part]
        return pl.ds(first, count), pl.ds(pl.multiple_of(l * TOK + first, 64), count)

    def acts_send(part, way):
        here, there = acts_rows(part)
        send(a_hbm.at[here, their_cols], ab.at[there, :], acts_out, acts_sem, way)

    def acts_got():
        got(ab.at[pl.ds(0, TOK), :], acts_sem)
        loads[5].wait()

    def pre_open():
        loads[1].wait()
        loads[2].wait()
        send(gpt.at[l], gpt.at[l], pre_out, pre_sem, inner)
        send(upt.at[l], upt.at[l], pre_out, pre_sem, inner)
        acts_send(1, inner)

    def own_gate_up():
        loads[3].wait()
        wg[own_rows, :] = gu3[...].reshape(ROWS, FG)

    def factors(group, rows):
        gate = jnp.transpose(gpt[group].astype(F32))
        up = jnp.transpose(upt[group].astype(F32))
        sig = jax.nn.sigmoid(gate)
        silu = gate * sig
        silu_s[rows, :] = silu
        dgate_s[rows, :] = up * sig * (1.0 + gate * (1.0 - sig))
        hid[rows, :] = (silu * up).astype(BF)

    def their_factors():
        got(gpt, pre_sem)
        factors(1 - l, theirs)

    def packed_at(group, quarter, count):
        return pl.multiple_of(group * (TOK * 7 // 2) + quarter * (QT * 7 // 2), 32), count * 7 // 2

    def product(group, quarter, count, part, sem):
        rows = pl.ds(pl.multiple_of(group * TOK + quarter * QT, QT), count)
        ghf[rows, :] = part
        first, size = packed_at(group, quarter, count)
        pack(ghs, first, part)
        block = pl.ds(first, size)
        send(ghs.at[block, :], ghr.at[block, :], product_out, sem, inner)

    def slab_product(xs):
        where = pl.ds(pl.multiple_of(xs * SLAB, 128), SLAB)
        return jnp.dot(gb[mine, where], wd[where, :], preferred_element_type=F32)

    def own_product():
        loads[4].wait()
        for k in range(3):
            down.side_got(k)
        part = slab_product(x) + slab_product(xm) + slab_product(xp)
        down.side_got(3)
        product(l, 0, TOK, part + slab_product(xo), own_sem)

    def quarter_rows(group, k):
        return pl.ds(pl.multiple_of(group * TOK + quarters[k] * QT, QT), QT)

    def quarter_product(k):
        rows = quarter_rows(1 - l, k)
        product(1 - l, quarters[k], QT, jnp.dot(gb[rows, :], wd[...], preferred_element_type=F32), quarter_sem)

    def near_products():
        outs.near_got()
        quarter_product(1)
        quarter_product(2)

    def far_product():
        outs.far_got()
        quarter_product(3)

    order = (xo, xp, xm, x)

    def own(core):
        return pl.ds(pl.multiple_of(core * ROWS, 32), ROWS)

    class Grad:
        def __init__(self, left, right, mat, recv, pair, near1, near2, out):
            self.left, self.right = left, right
            self.mat, self.recv, self.pair = mat, recv, pair
            self.near1, self.near2, self.out = near1, near2, out
            self.like = wd if right is hid else wg
            self.outlet = outlets.block()
            self.early, self.late, self.first, self.rest = (sems.block() for _ in range(4))

        def got(self, rows, sem):
            got(self.like.at[pl.ds(0, rows), :], sem)

        def put(self, src, dst, sem, to):
            send(src, dst, self.outlet, sem, to)

        def drain(self):
            gone(self.like.at[pl.ds(0, 7 * ROWS), :], self.outlet)

        def multiply(self, k):
            xs = order[k]
            self.mat[k] = wgrad_slab(self.left, self.right, xs).astype(BF)
            self.put(self.mat.at[k, own(1 - c), :], self.recv.at[k], self.late if k == 3 else self.early, sib)

        def pair_sum(self, k):
            return self.mat[k, own(c), :].astype(F32) + self.recv[k].astype(F32)

        def start(self):
            lo, hi = pl.ds(0, HALF), pl.ds(HALF, HALF)
            self.got(3 * ROWS, self.early)
            self.pair[0] = self.pair_sum(0).astype(BF)
            self.put(self.pair.at[0, lo, :], self.near1.at[0], self.first, to_xp)
            self.put(self.pair.at[0, hi, :], self.near1.at[1], self.first, to_xm)
            self.pair[1] = self.pair_sum(1).astype(BF)
            self.put(self.pair.at[1, hi, :], self.near2.at[0, hi, :], self.rest, to_xp)
            self.pair[2] = self.pair_sum(2).astype(BF)
            self.put(self.pair.at[2, lo, :], self.near2.at[1, lo, :], self.rest, to_xm)

        def relay(self):
            lo, hi = pl.ds(0, HALF), pl.ds(HALF, HALF)
            self.got(ROWS, self.first)
            self.pair[1, lo, :] = (self.pair[1, lo, :].astype(F32) + self.near1[0].astype(F32)).astype(BF)
            self.put(self.pair.at[1, lo, :], self.near2.at[0, lo, :], self.rest, to_xp)
            self.pair[2, hi, :] = (self.pair[2, hi, :].astype(F32) + self.near1[1].astype(F32)).astype(BF)
            self.put(self.pair.at[2, hi, :], self.near2.at[1, hi, :], self.rest, to_xm)

        def finish(self):
            self.got(ROWS, self.late)
            total = self.pair_sum(3)
            self.got(2 * ROWS, self.rest)
            total = total + self.near2[0].astype(F32) + self.near2[1].astype(F32)
            total = total * (1.0 / 16.0)
            if self.out.ndim == 3:
                self.out[:, 0, :] = total[:, :FD]
                self.out[:, 1, :] = total[:, FD:]
            else:
                self.out[...] = total

    grad_down = Grad(gb, hid, dws_d, dwr_d, vs_d, r1_d, r2_d, wd_out)
    grad_gate = Grad(ab, ghb, dws_g, dwr_g, vs_g, r1_g, r2_g, wg_out)

    def hidden_grads(group, quarter, count):
        rows = pl.ds(pl.multiple_of(group * TOK + quarter * QT, QT), count)
        total = ghf[rows, :] + unpack(ghr, packed_at(group, quarter, count)[0], count).astype(F32)
        ghb[rows, pl.ds(0, FD)] = (total * dgate_s[rows, :]).astype(BF)
        ghb[rows, pl.ds(FD, FD)] = (total * silu_s[rows, :]).astype(BF)

    def their_grads():
        got(ghr.at[pl.ds(0, TOK * 7 // 2), :], own_sem)
        hidden_grads(1 - l, 0, TOK)

    def my_grads():
        got(ghr.at[pl.ds(0, TOK * 7 // 2), :], quarter_sem)
        for k in range(4):
            hidden_grads(l, k, QT)

    slabs = [(x, xm, xp, xo)[k] for k, _ in CHUNKS]
    kinds = [kind for _, kind in CHUNKS]
    y_sum = [(sems.block(), sems.block()) for _ in range(8)]
    z_sum = [sems.block() for _ in range(8)]
    z_all = [(sems.block(), sems.block()) for _ in range(8)]
    y_all = [(sems.block(), sems.block()) for _ in range(8)]
    y_sum_out, z_sum_out, z_all_out, y_all_out = (outlets.block() for _ in range(4))

    def ways(i):
        if i % 2 == 0:
            return (to_yp, yp), (to_ym, ym)
        return (to_ym, ym), (to_yp, yp)

    def stage0(i):
        k, kind = CHUNKS[i]
        if all(CHUNKS[e][0] != k for e in range(i)):
            gate_up.side_got(k)
        rows = pl.ds(pl.multiple_of(slabs[i] * SLAB, 128), SLAB)
        prod = lax.dot_general(
            ghb[theirs if kind == 0 else mine, :],
            wg[rows, :],
            (((1,), (1,)), ((), ())),
            preferred_element_type=F32,
        )
        pb[i] = prod.astype(BF).reshape(4, QT, SLAB)
        (ahead, ahead_y), (behind, behind_y) = ways(i)
        first, rest = y_sum[i]
        if i in DIRECT_SUM:
            send(pb.at[i, yo], r1.at[i], y_sum_out, rest, {Y: yo})
            send(pb.at[i, ahead_y], r2.at[i], y_sum_out, rest, ahead)
        else:
            send(pb.at[i, yo], r1.at[i], y_sum_out, first, ahead)
        send(pb.at[i, behind_y], r3.at[i], y_sum_out, rest, behind)

    def stage1(i):
        if i in DIRECT_SUM:
            return
        (ahead, ahead_y), _ = ways(i)
        first, rest = y_sum[i]
        got(r1.at[i], first)
        pb[i, ahead_y] = (pb[i, ahead_y].astype(F32) + r1[i].astype(F32)).astype(BF)
        send(pb.at[i, ahead_y], r2.at[i], y_sum_out, rest, ahead)

    def stage2(i):
        total = pb[i, y].astype(F32)
        got(pb.at[0, pl.ds(0, 3 if i in DIRECT_SUM else 2)], y_sum[i][1])
        if i in DIRECT_SUM:
            total = total + r1[i].astype(F32)
        yb[i] = (total + r2[i].astype(F32) + r3[i].astype(F32)).astype(BF)
        for j in (2, 1, 3, 0):
            to = cross[j] if kinds[i] == 0 else along[j]
            if to is not None:
                rows = pl.ds(pl.multiple_of(((h + j) % 4) * HT, HT), HT)
                send(yb.at[i, rows, :], zr.at[i, j], z_sum_out, z_sum[i], to)

    def piece_of(i, first, count):
        half = 1 - l if kinds[i] == 0 else l
        return ob.at[slabs[i], half, pl.ds(pl.multiple_of(first, HT), count), :]

    def z_piece(i, which):
        return piece_of(i, y * QT + which * HT, HT)

    def quarter(i, which):
        return piece_of(i, which * QT, QT)

    def stage3(i):
        if kinds[i] == 0:
            got(zr.at[i], z_sum[i])
            total = zr[i, 0].astype(F32)
        else:
            got(zr.at[i, pl.ds(1, 3)], z_sum[i])
            total = yb[i, pl.ds(pl.multiple_of(h * HT, HT), HT), :].astype(F32)
        for j in range(1, 4):
            total = total + zr[i, j].astype(F32)
        piece = z_piece(i, h)
        piece[...] = total.astype(BF)
        first, rest = z_all[i]
        if i in DIRECT_SPREAD:
            first = rest
            send(piece, piece, z_all_out, rest, along[2])
        turn = (first, rest) if i % 2 == 0 else (rest, first)
        send(piece, piece, z_all_out, turn[0], along[1])
        send(piece, piece, z_all_out, turn[1], along[3])

    def stage4(i):
        if i in DIRECT_SPREAD:
            return
        behind, to = (hm, along[1]) if i % 2 == 0 else (hp, along[3])
        first, rest = z_all[i]
        piece = z_piece(i, behind)
        got(piece, first)
        send(piece, piece, z_all_out, rest, to)

    def stage5(i):
        got(zr.at[0, pl.ds(0, 3 if i in DIRECT_SPREAD else 2)], z_all[i][1])
        (ahead, _), (behind, _) = ways(i)
        first, rest = y_all[i]
        send(quarter(i, y), quarter(i, y), y_all_out, first, ahead)
        send(quarter(i, y), quarter(i, y), y_all_out, rest, behind)

    def stage6(i):
        (ahead, _), (_, behind_y) = ways(i)
        first, rest = y_all[i]
        got(quarter(i, behind_y), first)
        send(quarter(i, behind_y), quarter(i, behind_y), y_all_out, rest, ahead)

    def stage7(i):
        got(pb.at[0, pl.ds(0, 2)], y_all[i][1])

    steps = (
        lambda: outs.open(g_hbm, outer),
        down.open,
        pre_open,
        lambda: acts_send(0, outer),
        own_gate_up,
        lambda: factors(l, mine),
        down.forward,
        gate_up.open,
        down.near,
        their_factors,
        down.far,
        own_product,
        lambda: quarter_product(0),
        near_products,
        gate_up.forward,
        far_product,
        gate_up.near,
        gate_up.far,
        their_grads,
        my_grads,
        grad_down.start,
        grad_down.relay,
        grad_down.finish,
        grad_gate.start,
        grad_gate.relay,
        grad_gate.finish,
        grad_down.multiply,
        lambda k: (acts_got() if k == 0 else None, grad_gate.multiply(k)),
        outs.spread,
        outs.forward,
    )
    stages = (stage0, stage1, stage2, stage3, stage4, stage5, stage6, stage7)
    assert (outlets.n, sems.n) == (OUTLETS, INLETS), (outlets.n, sems.n)
    for code in ORDER:
        with jax.named_scope(f"{code}"):
            if code >= 100:
                stages[code // 10 - 10](code % 10)
            elif code >= 40:
                steps[code // 10 + 22](code % 10)
            else:
                steps[code]()

    with jax.named_scope("sends"):
        for part in (down, gate_up, grad_down, grad_gate):
            part.drain()
        gone(gb.at[pl.ds(0, TOK), :], outs.outlet)
        gone(ab.at[pl.ds(0, TOK), :], acts_out)
        gone(gpt, pre_out)
        gone(ghs, product_out)
        gone(pb.at[pl.ds(0, 6)], y_sum_out)
        gone(pb.at[pl.ds(0, 6)], y_all_out)
        gone(zr.at[pl.ds(0, 7)], z_sum_out)
        gone(zr.at[pl.ds(0, 6)], z_all_out)


def finish(ob, wg, wd, gi_hbm, wg_hbm, wd_hbm, sem):
    copies = [pltpu.make_async_copy(wg, wg_hbm, sem.at[8]), pltpu.make_async_copy(wd, wd_hbm, sem.at[9])]
    for k in range(8):
        cols = pl.ds((k % 2) * DH + (k // 2) * SLAB, SLAB)
        copies.append(pltpu.make_async_copy(ob.at[k // 2, k % 2], gi_hbm.at[:, cols], sem.at[k]))
    for made in copies:
        made.start()
    for made in copies:
        made.wait()


def per_device(activations, grad_out, gate_pre, up_pre, gate_up, down_weight):
    hbm = pl.BlockSpec(memory_space=pl.ANY)
    vmem = pl.BlockSpec(memory_space=pltpu.VMEM)
    scratch = [
        pltpu.VMEM((ROWS, 2, FD), BF),
        pltpu.VMEM((ROWS, FD), BF),
        pltpu.VMEM((16, HALF * 7 // 2, 128), BF),
        pltpu.VMEM((2 * TOK, DH), BF),
        pltpu.VMEM((2 * TOK, DH), BF),
        pltpu.VMEM((DH, FD), BF),
        pltpu.VMEM((DH, FG), BF),
        pltpu.VMEM((2, FD, TOK), BF),
        pltpu.VMEM((2, FD, TOK), BF),
        pltpu.VMEM((2 * TOK, FD), F32),
        pltpu.VMEM((TOK * 7, 128), BF),
        pltpu.VMEM((TOK * 7, 128), BF),
        pltpu.VMEM((2 * TOK, FD), F32),
        pltpu.VMEM((2 * TOK, FD), F32),
        pltpu.VMEM((2 * TOK, FD), BF),
        pltpu.VMEM((2 * TOK, FG), BF),
        pltpu.VMEM((4, SLAB, FD), BF),
        pltpu.VMEM((4, ROWS, FD), BF),
        pltpu.VMEM((4, SLAB, FG), BF),
        pltpu.VMEM((4, ROWS, FG), BF),
        pltpu.VMEM((3, ROWS, FD), BF),
        pltpu.VMEM((3, ROWS, FG), BF),
        pltpu.VMEM((2, HALF, FD), BF),
        pltpu.VMEM((2, HALF, FG), BF),
        pltpu.VMEM((2, ROWS, FD), BF),
        pltpu.VMEM((2, ROWS, FG), BF),
        pltpu.VMEM((8, 4, QT, SLAB), BF),
        pltpu.VMEM((8, QT, SLAB), BF),
        pltpu.VMEM((8, QT, SLAB), BF),
        pltpu.VMEM((8, QT, SLAB), BF),
        pltpu.VMEM((8, QT, SLAB), BF),
        pltpu.VMEM((8, 4, HT, SLAB), BF),
        pltpu.SemaphoreType.DMA((6,)),
        pltpu.SemaphoreType.DMA((OUTLETS,)),
        pltpu.SemaphoreType.DMA((INLETS,)),
    ]
    held = pl.pallas_call(
        kernel,
        out_shape=(
            pltpu.VMEM((4, 2, TOK, SLAB), BF),
            pltpu.VMEM((ROWS, 2, FD), F32),
            pltpu.VMEM((ROWS, FD), F32),
        ),
        in_specs=[hbm] * 6,
        out_specs=(vmem, vmem, vmem),
        scratch_shapes=scratch,
        compiler_params=pltpu.CompilerParams(
            collective_id=0, has_side_effects=True, vmem_limit_bytes=56 * 1024 * 1024
        ),
        name="step",
    )(activations, grad_out, gate_pre.T, up_pre.T, gate_up, down_weight)
    held = [pltpu.with_memory_space_constraint(v, pltpu.VMEM) for v in held]
    return pl.pallas_call(
        finish,
        out_shape=(
            jax.ShapeDtypeStruct((TOK, D), BF),
            jax.ShapeDtypeStruct((ROWS, 2, FD), F32),
            jax.ShapeDtypeStruct((ROWS, FD), F32),
        ),
        in_specs=[vmem] * 3,
        out_specs=(hbm, hbm, hbm),
        scratch_shapes=[pltpu.SemaphoreType.DMA((10,))],
        compiler_params=pltpu.CompilerParams(vmem_limit_bytes=4 * 1024 * 1024),
        name="finish",
    )(*held)


def solution(mesh):
    split = Mesh(mesh.devices.reshape(2, 4, 2, 4, 4), (Z, X, C, H, Y))
    return jax.shard_map(
        per_device,
        mesh=split,
        in_specs=(
            P(DP, None),
            P(DP, None),
            P(DP, TENSOR),
            P(DP, TENSOR),
            P(DP, None, TENSOR),
            P(DP, TENSOR),
        ),
        out_specs=(P(DP, None), P(DP, None, TENSOR), P(DP, TENSOR)),
        check_vma=False,
    )
```

```python
import jax
import jax.numpy as jnp
from jax import lax
from jax.experimental import pallas as pl
from jax.experimental.pallas import tpu as pltpu
from jax.sharding import Mesh
from jax.sharding import PartitionSpec as P

Z, X, C, H, Y = "dp_0", "dp_1", "dp_2", "tensor_0", "tensor_1"
DP = (Z, X, C)
TENSOR = (H, Y)
BF = jnp.bfloat16
F32 = jnp.float32

TOK = 256
D = 5120
DH = D // 2
SLAB = 640
ROWS = 320
HALF = 160
FD = 448
FG = 896
QT = 64
HT = 16

OUTLETS, INLETS = 12, 88
CHUNKS = ((0, 0), (1, 0), (2, 0), (0, 1), (1, 1), (2, 1), (3, 0), (3, 1))
DIRECT_SUM = (0, 1)
DIRECT_SPREAD = (0, 1, 5, 6, 7)
ORDER = (
    1, 2, 0, 3, 6, 60, 4, 7, 8, 61, 10, 70, 5, 11, 71, 13, 14, 9, 12, 15, 18, 100, 16, 40, 41, 42, 101, 102, 19,
    43, 20, 17, 103, 104, 120, 50, 121, 51, 112, 105, 21, 130, 113, 114, 131, 106, 122, 115, 52, 123, 107, 22,
    124, 23, 116, 151, 132, 125, 117, 150, 133, 142, 134, 126, 143, 127, 161, 53, 152, 144, 160, 135, 24, 136,
    153, 154, 137, 171, 155, 156, 162, 164, 170, 157, 163, 25, 165, 166, 167, 173, 174, 175, 172, 177, 176,
)


def pack(ref, first, value):
    n = value.shape[0]
    value = value.astype(BF)
    for tile in range(3):
        ref[pl.ds(first + tile * n, n), :] = value[:, tile * 128 : (tile + 1) * 128]
    tail = value[:, 384:]
    ref[pl.ds(first + 3 * n, n // 2), :] = jnp.concatenate([tail[: n // 2], tail[n // 2 :]], axis=1)


def unpack(ref, first, n):
    tiles = [ref[pl.ds(first + tile * n, n), :] for tile in range(3)]
    tail = ref[pl.ds(first + 3 * n, n // 2), :]
    return jnp.concatenate(tiles + [jnp.concatenate([tail[:, :64], tail[:, 64:]], axis=0)], axis=1)


class Sems:
    def __init__(self):
        self.n = 0

    def block(self, count=1):
        first = self.n
        self.n += count
        return first


def wgrad_slab(acts, right, xs):
    cols = pl.ds(pl.multiple_of(xs * SLAB, 128), SLAB)
    return lax.dot_general(
        acts[:, cols], right[...], (((0,), (0,)), ((), ())), preferred_element_type=F32
    )


def kernel(
    a_hbm,
    g_hbm,
    gp_hbm,
    up_hbm,
    gu_hbm,
    dn_hbm,
    ob,
    wg_out,
    wd_out,
    gu3,
    dnb,
    wp,
    gb,
    ab,
    wd,
    wg,
    gpt,
    upt,
    ghf,
    ghs,
    ghr,
    silu_s,
    dgate_s,
    hid,
    ghb,
    dws_d,
    dwr_d,
    dws_g,
    dwr_g,
    vs_d,
    vs_g,
    r1_d,
    r1_g,
    r2_d,
    r2_g,
    pb,
    r1,
    r2,
    r3,
    yb,
    zr,
    lsem,
    ss,
    rs,
):
    l, x, c, h, y = (lax.axis_index(n) for n in (Z, X, C, H, Y))
    xp, xm, xo = (x + 1) % 4, (x + 3) % 4, (x + 2) % 4
    yp, ym, yo = (y + 1) % 4, (y + 3) % 4, (y + 2) % 4
    to_xp, to_xm = {X: xp}, {X: xm}
    to_yp, to_ym = {Y: yp}, {Y: ym}
    hp, hm, ho = (h + 1) % 4, (h + 3) % 4, (h + 2) % 4
    sib = {C: 1 - c}
    inner = {Z: 1 - l}
    outer = {Z: 1 - l, H: (h + 2 * l + 3) % 4}
    cross = [{Z: 1 - l, H: (h + j) % 4} for j in range(4)]
    along = [None] + [{H: (h + j) % 4} for j in range(1, 4)]
    sems, outlets = Sems(), Sems()

    def copy(src, dst, outlet, sem, to):
        return pltpu.make_async_remote_copy(
            src_ref=src,
            dst_ref=dst,
            send_sem=ss.at[outlet],
            recv_sem=rs.at[sem],
            device_id=to,
            device_id_type=pl.DeviceIdType.MESH,
        )

    def send(src, dst, outlet, sem, to):
        copy(src, dst, outlet, sem, to).start()

    def got(like, sem):
        copy(like, like, 0, sem, sib).wait_recv()

    def gone(like, outlet):
        copy(like, like, outlet, 0, sib).wait_send()

    mine = pl.ds(pl.multiple_of(l * TOK, TOK), TOK)
    theirs = pl.ds(pl.multiple_of((1 - l) * TOK, TOK), TOK)
    my_cols = pl.ds(pl.multiple_of(l * DH, 128), DH)
    their_cols = pl.ds(pl.multiple_of((1 - l) * DH, 128), DH)

    def slab_rows(xs, core, part=None):
        start = xs * SLAB + core * ROWS
        if part is None:
            return pl.ds(pl.multiple_of(start, 32), ROWS)
        return pl.ds(pl.multiple_of(start + part * HALF, 32), HALF)

    barrier = pltpu.get_barrier_semaphore()
    greeted = [to_xp, to_xm, to_yp, to_ym, sib] + cross + along[1:]
    for peer in greeted:
        pl.semaphore_signal(barrier, inc=1, device_id=peer, device_id_type=pl.DeviceIdType.MESH)

    own_rows = slab_rows(x, c)
    loads = [
        pltpu.make_async_copy(dn_hbm, dnb, lsem.at[0]),
        pltpu.make_async_copy(gp_hbm, gpt.at[l], lsem.at[1]),
        pltpu.make_async_copy(up_hbm, upt.at[l], lsem.at[2]),
        pltpu.make_async_copy(gu_hbm, gu3, lsem.at[3]),
        pltpu.make_async_copy(g_hbm.at[:, my_cols], gb.at[mine, :], lsem.at[4]),
        pltpu.make_async_copy(a_hbm.at[:, my_cols], ab.at[mine, :], lsem.at[5]),
    ]
    for load in loads:
        load.start()
    loads[0].wait()
    for part in range(2):
        pack(wp.at[4 * x + 2 * c + part], 0, dnb[pl.ds(part * HALF, HALF), :])
    wd[own_rows, :] = dnb[...]
    pl.semaphore_wait(barrier, len(greeted))

    class Weights:
        def __init__(self, ref):
            self.ref = ref
            self.outlet = outlets.block()
            self.first, self.second, self.last = sems.block(), sems.block(), sems.block()
            self.side = [sems.block() for _ in range(4)]

        def block(self, xs, core, part=None):
            return self.ref.at[slab_rows(xs, core, part), :]

        def like(self, halves):
            return self.ref.at[pl.ds(0, halves * HALF), :]

        def ready(self, xs, core):
            pass

        def put(self, block, sem, to):
            send(block, block, self.outlet, sem, to)

        def open(self):
            self.put(self.block(x, c, 0), self.first, to_xp)
            self.put(self.block(x, c, 1), self.first, to_xm)
            self.put(self.block(x, c, 1), self.second, to_xp)
            self.put(self.block(x, c, 0), self.second, to_xm)
            self.put(self.block(x, c), self.side[0], sib)

        def forward(self):
            got(self.like(2), self.first)
            self.put(self.block(xm, c, 0), self.last, to_xp)
            self.put(self.block(xp, c, 1), self.last, to_xm)

        def near(self):
            got(self.like(2), self.second)
            self.put(self.block(xm, c), self.side[1], sib)
            self.put(self.block(xp, c), self.side[2], sib)
            self.ready(xm, c)
            self.ready(xp, c)

        def far(self):
            got(self.like(2), self.last)
            self.put(self.block(xo, c), self.side[3], sib)
            self.ready(xo, c)

        def side_got(self, k):
            got(self.like(2), self.side[k])
            self.ready((x, xm, xp, xo)[k], 1 - c)

        def drain(self):
            gone(self.like(14), self.outlet)

    class Packed(Weights):
        def block(self, xs, core, part=None):
            first = 4 * xs + 2 * core
            return wp.at[pl.ds(first, 2)] if part is None else wp.at[first + part]

        def like(self, halves):
            return wp.at[pl.ds(0, halves)]

        def ready(self, xs, core):
            for part in range(2):
                self.ref[slab_rows(xs, core, part), :] = unpack(self.block(xs, core, part), 0, HALF)

    class Tokens:
        def __init__(self, ref):
            self.ref = ref
            self.outlet = outlets.block()
            self.over = sems.block(2)
            self.plus, self.minus = sems.block(), sems.block()
            self.near, self.far = sems.block(), sems.block()

        def at(self, group, quarter, part=None):
            start = group * TOK + quarter * QT
            if part is None:
                return self.ref.at[pl.ds(pl.multiple_of(start, 32), QT), :]
            return self.ref.at[pl.ds(pl.multiple_of(start + part * 32, 32), 32), :]

        def open(self, hbm, way):
            for part in range(2):
                rows = pl.ds(pl.multiple_of(y * QT + part * 32, 32), 32)
                send(hbm.at[rows, their_cols], self.at(l, y, part), self.outlet, self.over + part, way)

        def put(self, piece, sem, to):
            send(piece, piece, self.outlet, sem, to)

        def spread(self, part):
            piece = self.at(1 - l, y, part)
            got(piece, self.over + part)
            if part == 0:
                self.put(piece, self.plus, to_yp)
                self.put(piece, self.near, to_ym)
            else:
                self.put(piece, self.minus, to_ym)
                self.put(piece, self.near, to_yp)

        def forward(self, part):
            piece = self.at(1 - l, (ym, yp)[part], part)
            got(piece, (self.plus, self.minus)[part])
            self.put(piece, self.far, (to_yp, to_ym)[part])

        def near_got(self):
            got(self.ref.at[pl.ds(0, QT), :], self.near)

        def far_got(self):
            got(self.ref.at[pl.ds(0, QT), :], self.far)

    down, gate_up = Packed(wd), Weights(wg)
    outs = Tokens(gb)
    acts_sem, pre_sem, own_sem, quarter_sem = (sems.block() for _ in range(4))
    acts_out, pre_out, product_out = (outlets.block() for _ in range(3))
    quarters = (y, ym, yp, yo)

    def acts_rows(part):
        first, count = ((0, 192), (192, 64))[part]
        return pl.ds(first, count), pl.ds(pl.multiple_of(l * TOK + first, 64), count)

    def acts_send(part, way):
        here, there = acts_rows(part)
        send(a_hbm.at[here, their_cols], ab.at[there, :], acts_out, acts_sem, way)

    def acts_got():
        got(ab.at[pl.ds(0, TOK), :], acts_sem)
        loads[5].wait()

    def pre_open():
        loads[1].wait()
        loads[2].wait()
        send(gpt.at[l], gpt.at[l], pre_out, pre_sem, inner)
        send(upt.at[l], upt.at[l], pre_out, pre_sem, inner)
        acts_send(1, inner)

    def own_gate_up():
        loads[3].wait()
        wg[own_rows, :] = gu3[...].reshape(ROWS, FG)

    def factors(group, rows):
        gate = jnp.transpose(gpt[group].astype(F32))
        up = jnp.transpose(upt[group].astype(F32))
        sig = jax.nn.sigmoid(gate)
        silu = gate * sig
        silu_s[rows, :] = silu
        dgate_s[rows, :] = up * sig * (1.0 + gate * (1.0 - sig))
        hid[rows, :] = (silu * up).astype(BF)

    def their_factors():
        got(gpt, pre_sem)
        factors(1 - l, theirs)

    def packed_at(group, quarter, count):
        return pl.multiple_of(group * (TOK * 7 // 2) + quarter * (QT * 7 // 2), 32), count * 7 // 2

    def product(group, quarter, count, part, sem):
        rows = pl.ds(pl.multiple_of(group * TOK + quarter * QT, QT), count)
        ghf[rows, :] = part
        first, size = packed_at(group, quarter, count)
        pack(ghs, first, part)
        block = pl.ds(first, size)
        send(ghs.at[block, :], ghr.at[block, :], product_out, sem, inner)

    def slab_product(xs):
        where = pl.ds(pl.multiple_of(xs * SLAB, 128), SLAB)
        return jnp.dot(gb[mine, where], wd[where, :], preferred_element_type=F32)

    def own_product():
        loads[4].wait()
        for k in range(3):
            down.side_got(k)
        part = slab_product(x) + slab_product(xm) + slab_product(xp)
        down.side_got(3)
        product(l, 0, TOK, part + slab_product(xo), own_sem)

    def quarter_rows(group, k):
        return pl.ds(pl.multiple_of(group * TOK + quarters[k] * QT, QT), QT)

    def quarter_product(k):
        rows = quarter_rows(1 - l, k)
        product(1 - l, quarters[k], QT, jnp.dot(gb[rows, :], wd[...], preferred_element_type=F32), quarter_sem)

    def near_products():
        outs.near_got()
        quarter_product(1)
        quarter_product(2)

    def far_product():
        outs.far_got()
        quarter_product(3)

    order = (xo, xp, xm, x)

    def own(core):
        return pl.ds(pl.multiple_of(core * ROWS, 32), ROWS)

    class Grad:
        def __init__(self, left, right, mat, recv, pair, near1, near2, out):
            self.left, self.right = left, right
            self.mat, self.recv, self.pair = mat, recv, pair
            self.near1, self.near2, self.out = near1, near2, out
            self.like = wd if right is hid else wg
            self.outlet = outlets.block()
            self.early, self.late, self.first, self.rest = (sems.block() for _ in range(4))

        def got(self, rows, sem):
            got(self.like.at[pl.ds(0, rows), :], sem)

        def put(self, src, dst, sem, to):
            send(src, dst, self.outlet, sem, to)

        def drain(self):
            gone(self.like.at[pl.ds(0, 7 * ROWS), :], self.outlet)

        def multiply(self, k):
            xs = order[k]
            self.mat[k] = wgrad_slab(self.left, self.right, xs).astype(BF)
            self.put(self.mat.at[k, own(1 - c), :], self.recv.at[k], self.late if k == 3 else self.early, sib)

        def pair_sum(self, k):
            return self.mat[k, own(c), :].astype(F32) + self.recv[k].astype(F32)

        def start(self):
            lo, hi = pl.ds(0, HALF), pl.ds(HALF, HALF)
            self.got(3 * ROWS, self.early)
            self.pair[0] = self.pair_sum(0).astype(BF)
            self.put(self.pair.at[0, lo, :], self.near1.at[0], self.first, to_xp)
            self.put(self.pair.at[0, hi, :], self.near1.at[1], self.first, to_xm)
            self.pair[1] = self.pair_sum(1).astype(BF)
            self.put(self.pair.at[1, hi, :], self.near2.at[0, hi, :], self.rest, to_xp)
            self.pair[2] = self.pair_sum(2).astype(BF)
            self.put(self.pair.at[2, lo, :], self.near2.at[1, lo, :], self.rest, to_xm)

        def relay(self):
            lo, hi = pl.ds(0, HALF), pl.ds(HALF, HALF)
            self.got(ROWS, self.first)
            self.pair[1, lo, :] = (self.pair[1, lo, :].astype(F32) + self.near1[0].astype(F32)).astype(BF)
            self.put(self.pair.at[1, lo, :], self.near2.at[0, lo, :], self.rest, to_xp)
            self.pair[2, hi, :] = (self.pair[2, hi, :].astype(F32) + self.near1[1].astype(F32)).astype(BF)
            self.put(self.pair.at[2, hi, :], self.near2.at[1, hi, :], self.rest, to_xm)

        def finish(self):
            self.got(ROWS, self.late)
            total = self.pair_sum(3)
            self.got(2 * ROWS, self.rest)
            total = total + self.near2[0].astype(F32) + self.near2[1].astype(F32)
            total = total * (1.0 / 16.0)
            if self.out.ndim == 3:
                self.out[:, 0, :] = total[:, :FD]
                self.out[:, 1, :] = total[:, FD:]
            else:
                self.out[...] = total

    grad_down = Grad(gb, hid, dws_d, dwr_d, vs_d, r1_d, r2_d, wd_out)
    grad_gate = Grad(ab, ghb, dws_g, dwr_g, vs_g, r1_g, r2_g, wg_out)

    def hidden_grads(group, quarter, count):
        rows = pl.ds(pl.multiple_of(group * TOK + quarter * QT, QT), count)
        total = ghf[rows, :] + unpack(ghr, packed_at(group, quarter, count)[0], count).astype(F32)
        ghb[rows, pl.ds(0, FD)] = (total * dgate_s[rows, :]).astype(BF)
        ghb[rows, pl.ds(FD, FD)] = (total * silu_s[rows, :]).astype(BF)

    def their_grads():
        got(ghr.at[pl.ds(0, TOK * 7 // 2), :], own_sem)
        hidden_grads(1 - l, 0, TOK)

    def my_grads():
        got(ghr.at[pl.ds(0, TOK * 7 // 2), :], quarter_sem)
        for k in range(4):
            hidden_grads(l, k, QT)

    slabs = [(x, xm, xp, xo)[k] for k, _ in CHUNKS]
    kinds = [kind for _, kind in CHUNKS]
    y_sum = [(sems.block(), sems.block()) for _ in range(8)]
    z_sum = [sems.block() for _ in range(8)]
    z_all = [(sems.block(), sems.block()) for _ in range(8)]
    y_all = [(sems.block(), sems.block()) for _ in range(8)]
    y_sum_out, z_sum_out, z_all_out, y_all_out = (outlets.block() for _ in range(4))

    def ways(i):
        if i % 2 == 0:
            return (to_yp, yp), (to_ym, ym)
        return (to_ym, ym), (to_yp, yp)

    def stage0(i):
        k, kind = CHUNKS[i]
        if all(CHUNKS[e][0] != k for e in range(i)):
            gate_up.side_got(k)
        rows = pl.ds(pl.multiple_of(slabs[i] * SLAB, 128), SLAB)
        prod = lax.dot_general(
            ghb[theirs if kind == 0 else mine, :],
            wg[rows, :],
            (((1,), (1,)), ((), ())),
            preferred_element_type=F32,
        )
        pb[i] = prod.astype(BF).reshape(4, QT, SLAB)
        (ahead, ahead_y), (behind, behind_y) = ways(i)
        first, rest = y_sum[i]
        if i in DIRECT_SUM:
            send(pb.at[i, yo], r1.at[i], y_sum_out, rest, {Y: yo})
            send(pb.at[i, ahead_y], r2.at[i], y_sum_out, rest, ahead)
        else:
            send(pb.at[i, yo], r1.at[i], y_sum_out, first, ahead)
        send(pb.at[i, behind_y], r3.at[i], y_sum_out, rest, behind)

    def stage1(i):
        if i in DIRECT_SUM:
            return
        (ahead, ahead_y), _ = ways(i)
        first, rest = y_sum[i]
        got(r1.at[i], first)
        pb[i, ahead_y] = (pb[i, ahead_y].astype(F32) + r1[i].astype(F32)).astype(BF)
        send(pb.at[i, ahead_y], r2.at[i], y_sum_out, rest, ahead)

    def stage2(i):
        total = pb[i, y].astype(F32)
        got(pb.at[0, pl.ds(0, 3 if i in DIRECT_SUM else 2)], y_sum[i][1])
        if i in DIRECT_SUM:
            total = total + r1[i].astype(F32)
        yb[i] = (total + r2[i].astype(F32) + r3[i].astype(F32)).astype(BF)
        for j in (2, 1, 3, 0):
            to = cross[j] if kinds[i] == 0 else along[j]
            if to is not None:
                rows = pl.ds(pl.multiple_of(((h + j) % 4) * HT, HT), HT)
                send(yb.at[i, rows, :], zr.at[i, j], z_sum_out, z_sum[i], to)

    def piece_of(i, first, count):
        half = 1 - l if kinds[i] == 0 else l
        return ob.at[slabs[i], half, pl.ds(pl.multiple_of(first, HT), count), :]

    def z_piece(i, which):
        return piece_of(i, y * QT + which * HT, HT)

    def quarter(i, which):
        return piece_of(i, which * QT, QT)

    def stage3(i):
        if kinds[i] == 0:
            got(zr.at[i], z_sum[i])
            total = zr[i, 0].astype(F32)
        else:
            got(zr.at[i, pl.ds(1, 3)], z_sum[i])
            total = yb[i, pl.ds(pl.multiple_of(h * HT, HT), HT), :].astype(F32)
        for j in range(1, 4):
            total = total + zr[i, j].astype(F32)
        piece = z_piece(i, h)
        piece[...] = total.astype(BF)
        first, rest = z_all[i]
        if i in DIRECT_SPREAD:
            first = rest
            send(piece, piece, z_all_out, rest, along[2])
        turn = (first, rest) if i % 2 == 0 else (rest, first)
        send(piece, piece, z_all_out, turn[0], along[1])
        send(piece, piece, z_all_out, turn[1], along[3])

    def stage4(i):
        if i in DIRECT_SPREAD:
            return
        behind, to = (hm, along[1]) if i % 2 == 0 else (hp, along[3])
        first, rest = z_all[i]
        piece = z_piece(i, behind)
        got(piece, first)
        send(piece, piece, z_all_out, rest, to)

    def stage5(i):
        got(zr.at[0, pl.ds(0, 3 if i in DIRECT_SPREAD else 2)], z_all[i][1])
        (ahead, _), (behind, _) = ways(i)
        first, rest = y_all[i]
        send(quarter(i, y), quarter(i, y), y_all_out, first, ahead)
        send(quarter(i, y), quarter(i, y), y_all_out, rest, behind)

    def stage6(i):
        (ahead, _), (_, behind_y) = ways(i)
        first, rest = y_all[i]
        got(quarter(i, behind_y), first)
        send(quarter(i, behind_y), quarter(i, behind_y), y_all_out, rest, ahead)

    def stage7(i):
        got(pb.at[0, pl.ds(0, 2)], y_all[i][1])

    steps = (
        lambda: outs.open(g_hbm, outer),
        down.open,
        pre_open,
        lambda: acts_send(0, outer),
        own_gate_up,
        lambda: factors(l, mine),
        down.forward,
        gate_up.open,
        down.near,
        their_factors,
        down.far,
        own_product,
        lambda: quarter_product(0),
        near_products,
        gate_up.forward,
        far_product,
        gate_up.near,
        gate_up.far,
        their_grads,
        my_grads,
        grad_down.start,
        grad_down.relay,
        grad_down.finish,
        grad_gate.start,
        grad_gate.relay,
        grad_gate.finish,
        grad_down.multiply,
        lambda k: (acts_got() if k == 0 else None, grad_gate.multiply(k)),
        outs.spread,
        outs.forward,
    )
    stages = (stage0, stage1, stage2, stage3, stage4, stage5, stage6, stage7)
    assert (outlets.n, sems.n) == (OUTLETS, INLETS), (outlets.n, sems.n)
    for code in ORDER:
        with jax.named_scope(f"{code}"):
            if code >= 100:
                stages[code // 10 - 10](code % 10)
            elif code >= 40:
                steps[code // 10 + 22](code % 10)
            else:
                steps[code]()

    with jax.named_scope("sends"):
        for part in (down, gate_up, grad_down, grad_gate):
            part.drain()
        gone(gb.at[pl.ds(0, TOK), :], outs.outlet)
        gone(ab.at[pl.ds(0, TOK), :], acts_out)
        gone(gpt, pre_out)
        gone(ghs, product_out)
        gone(pb.at[pl.ds(0, 6)], y_sum_out)
        gone(pb.at[pl.ds(0, 6)], y_all_out)
        gone(zr.at[pl.ds(0, 7)], z_sum_out)
        gone(zr.at[pl.ds(0, 6)], z_all_out)


def finish(ob, wg, wd, gi_hbm, wg_hbm, wd_hbm, sem):
    copies = []
    for k in range(8):
        cols = pl.ds((k % 2) * DH + (k // 2) * SLAB, SLAB)
        copies.append(pltpu.make_async_copy(ob.at[k // 2, k % 2], gi_hbm.at[:, cols], sem.at[k]))
    copies += [pltpu.make_async_copy(wg, wg_hbm, sem.at[8]), pltpu.make_async_copy(wd, wd_hbm, sem.at[9])]
    for made in copies:
        made.start()
    for made in copies:
        made.wait()


def per_device(activations, grad_out, gate_pre, up_pre, gate_up, down_weight):
    hbm = pl.BlockSpec(memory_space=pl.ANY)
    vmem = pl.BlockSpec(memory_space=pltpu.VMEM)
    scratch = [
        pltpu.VMEM((ROWS, 2, FD), BF),
        pltpu.VMEM((ROWS, FD), BF),
        pltpu.VMEM((16, HALF * 7 // 2, 128), BF),
        pltpu.VMEM((2 * TOK, DH), BF),
        pltpu.VMEM((2 * TOK, DH), BF),
        pltpu.VMEM((DH, FD), BF),
        pltpu.VMEM((DH, FG), BF),
        pltpu.VMEM((2, FD, TOK), BF),
        pltpu.VMEM((2, FD, TOK), BF),
        pltpu.VMEM((2 * TOK, FD), F32),
        pltpu.VMEM((TOK * 7, 128), BF),
        pltpu.VMEM((TOK * 7, 128), BF),
        pltpu.VMEM((2 * TOK, FD), F32),
        pltpu.VMEM((2 * TOK, FD), F32),
        pltpu.VMEM((2 * TOK, FD), BF),
        pltpu.VMEM((2 * TOK, FG), BF),
        pltpu.VMEM((4, SLAB, FD), BF),
        pltpu.VMEM((4, ROWS, FD), BF),
        pltpu.VMEM((4, SLAB, FG), BF),
        pltpu.VMEM((4, ROWS, FG), BF),
        pltpu.VMEM((3, ROWS, FD), BF),
        pltpu.VMEM((3, ROWS, FG), BF),
        pltpu.VMEM((2, HALF, FD), BF),
        pltpu.VMEM((2, HALF, FG), BF),
        pltpu.VMEM((2, ROWS, FD), BF),
        pltpu.VMEM((2, ROWS, FG), BF),
        pltpu.VMEM((8, 4, QT, SLAB), BF),
        pltpu.VMEM((8, QT, SLAB), BF),
        pltpu.VMEM((8, QT, SLAB), BF),
        pltpu.VMEM((8, QT, SLAB), BF),
        pltpu.VMEM((8, QT, SLAB), BF),
        pltpu.VMEM((8, 4, HT, SLAB), BF),
        pltpu.SemaphoreType.DMA((6,)),
        pltpu.SemaphoreType.DMA((OUTLETS,)),
        pltpu.SemaphoreType.DMA((INLETS,)),
    ]
    held = pl.pallas_call(
        kernel,
        out_shape=(
            pltpu.VMEM((4, 2, TOK, SLAB), BF),
            pltpu.VMEM((ROWS, 2, FD), F32),
            pltpu.VMEM((ROWS, FD), F32),
        ),
        in_specs=[hbm] * 6,
        out_specs=(vmem, vmem, vmem),
        scratch_shapes=scratch,
        compiler_params=pltpu.CompilerParams(
            collective_id=0, has_side_effects=True, vmem_limit_bytes=56 * 1024 * 1024
        ),
        name="step",
    )(activations, grad_out, gate_pre.T, up_pre.T, gate_up, down_weight)
    held = [pltpu.with_memory_space_constraint(v, pltpu.VMEM) for v in held]
    return pl.pallas_call(
        finish,
        out_shape=(
            jax.ShapeDtypeStruct((TOK, D), BF),
            jax.ShapeDtypeStruct((ROWS, 2, FD), F32),
            jax.ShapeDtypeStruct((ROWS, FD), F32),
        ),
        in_specs=[vmem] * 3,
        out_specs=(hbm, hbm, hbm),
        scratch_shapes=[pltpu.SemaphoreType.DMA((10,))],
        compiler_params=pltpu.CompilerParams(vmem_limit_bytes=4 * 1024 * 1024),
        name="finish",
    )(*held)


def solution(mesh):
    split = Mesh(mesh.devices.reshape(2, 4, 2, 4, 4), (Z, X, C, H, Y))
    return jax.shard_map(
        per_device,
        mesh=split,
        in_specs=(
            P(DP, None),
            P(DP, None),
            P(DP, TENSOR),
            P(DP, TENSOR),
            P(DP, None, TENSOR),
            P(DP, TENSOR),
        ),
        out_specs=(P(DP, None), P(DP, None, TENSOR), P(DP, TENSOR)),
        check_vma=False,
    )
```
